128 devices in a mesh: dp: 4 (over y), col: 32 (over z, x, core).
Axes of the slice: x: 4, y: 4, z: 4, core: 2. Of those that a mesh axis runs over, the one named last changes fastest.
Arguments:
- tokens: bfloat16 [1536, 2304], P('dp', 'col'), may hold values from -6 to 6
- cotangent: bfloat16 [1536, 2304], P('dp', 'col'), may hold values from -6 to 6
- prefix: int32 [12], P('dp'), may hold values from 0 to 3
- gate_weight: bfloat16 [2304, 36864], P(None, 'col'), may hold values from -0.125 to 0.125
- up_weight: bfloat16 [2304, 36864], P(None, 'col'), may hold values from -0.125 to 0.125
- down_weight: bfloat16 [36864, 2304], P('col'), may hold values from -0.0625 to 0.0625
Outputs:
- output: bfloat16 [1536, 2304], P('dp', 'col')
- input_grad: bfloat16 [1536, 2304], P('dp', 'col')
- grad_gate: bfloat16 [2304, 36864], P('dp', 'col')
- grad_up: bfloat16 [2304, 36864], P('dp', 'col')
- grad_down: bfloat16 [36864, 2304], P('col', 'dp')
The draws below stay inside these ranges and needn't reach their ends.
All inputs are finite; a program needn't handle non-finite values.
Results may differ from the reference program's by a relative error of at most 0.017.
Values may be sent and summed in bfloat16 or wider, within the bound.
A program may use at most 128 MiB of HBM per device.

```python
import jax
import jax.numpy as jnp

D = 2304
FF = 36864
BLOCK = 128
TOK_DEV = 384
TOKENS = 1536
BLOCKS = 12
N_DP = 4


def set_ends(result, stream_key, smallest, high):
    place = [jax.random.randint(jax.random.fold_in(stream_key, axis), (), 0, length) for axis, length in enumerate(result.shape)]
    main_axis = result.shape.index(max(result.shape))
    neighbour = place[:main_axis] + [(place[main_axis] + 1) % result.shape[main_axis]] + place[main_axis + 1:]
    return result.at[tuple(place)].set(smallest).at[tuple(neighbour)].set(high)


def levels(own_key, extent, pieces, smallest, largest):
    gain = 1.0
    for axis_at, parts in pieces:
        steps = jax.random.uniform(jax.random.fold_in(jax.random.fold_in(own_key, 6), axis_at), (parts,), jnp.float32, smallest / len(pieces), largest / len(pieces))
        gain = gain * jnp.repeat(jnp.exp(steps), extent[axis_at] // parts).reshape((-1,) + (1,) * (len(extent) - 1 - axis_at))
    return gain


def centred(own_key, dims, scale, reach, cuts=(), held_as=jnp.bfloat16):
    result = jax.random.normal(own_key, dims, jnp.float32) * scale
    if len(cuts) > 0:
        result = levels(own_key, dims, cuts, -0.22, 0.18) * result
    return jnp.clip(result, min=-reach, max=reach).astype(held_as)


def setup_inputs(seed: int = 0) -> dict:
    streams_of = jax.random.split(jax.random.key(seed), 7)
    tokens = centred(streams_of[0], (TOKENS, D), 1.0, 6.0, ((0, 4), (1, 32)))
    cotangent = centred(streams_of[1], (TOKENS, D), 1.0, 6.0, ((0, 4), (1, 32)))
    prefix = set_ends(jax.random.randint(streams_of[2], (BLOCKS,), 0, 4), jax.random.fold_in(streams_of[2], 1), 0, 3).astype(jnp.int32)
    gate_weight = centred(streams_of[3], (D, FF), D ** -0.5, 0.125, ((1, 32),))
    up_weight = centred(streams_of[4], (D, FF), D ** -0.5, 0.125, ((1, 32),))
    down_weight = centred(streams_of[5], (FF, D), (FF // 4) ** -0.5, 0.0625, ((0, 32),))
    return {"tokens": tokens, "cotangent": cotangent, "prefix": prefix, "gate_weight": gate_weight, "up_weight": up_weight, "down_weight": down_weight}


def gelu_pair(value):
    scale = 0.7978845608028654
    inner = jnp.tanh(scale * (value + 0.044715 * value * value * value))
    act = 0.5 * value * (1.0 + inner)
    slope = 0.5 * (1.0 + inner) + 0.5 * value * (1.0 - inner * inner) * scale * (1.0 + 3.0 * 0.044715 * value * value)
    return act, slope


def matmul(left, right):
    return jnp.dot(left.astype(jnp.float32), right.astype(jnp.float32))


def reference(tokens, cotangent, prefix, gate_weight, up_weight, down_weight):
    widths = jnp.left_shift(jnp.int32(FF // 8), prefix.astype(jnp.int32))
    per_token = jnp.repeat(widths, BLOCK, total_repeat_length=TOKENS)
    columns = jnp.arange(FF, dtype=jnp.int32)
    mask = (columns[None, :] < per_token[:, None]).astype(jnp.float32)
    gate = matmul(tokens, gate_weight)
    up = matmul(tokens, up_weight)
    act, slope = gelu_pair(gate)
    hidden = (mask * act * up).astype(jnp.bfloat16)
    output = matmul(hidden, down_weight).astype(jnp.bfloat16)
    back = matmul(cotangent, down_weight.T)
    dgate = (mask * back * up * slope).astype(jnp.bfloat16)
    dup = (mask * back * act).astype(jnp.bfloat16)
    input_grad = (matmul(dgate, gate_weight.T) + matmul(dup, up_weight.T)).astype(jnp.bfloat16)
    sum_gate = jnp.zeros((D, FF), jnp.float32)
    sum_up = jnp.zeros((D, FF), jnp.float32)
    sum_down = jnp.zeros((FF, D), jnp.float32)
    for group in range(N_DP):
        first = group * TOK_DEV
        last = first + TOK_DEV
        sum_gate = sum_gate + matmul(tokens[first:last].T, dgate[first:last]).astype(jnp.bfloat16).astype(jnp.float32)
        sum_up = sum_up + matmul(tokens[first:last].T, dup[first:last]).astype(jnp.bfloat16).astype(jnp.float32)
        sum_down = sum_down + matmul(hidden[first:last].T, cotangent[first:last]).astype(jnp.bfloat16).astype(jnp.float32)
    return (output, input_grad, sum_gate.astype(jnp.bfloat16), sum_up.astype(jnp.bfloat16), sum_down.astype(jnp.bfloat16))
```

```python
import functools

import jax
import jax.numpy as jnp
from jax import lax
from jax.experimental import pallas as pl
from jax.experimental.pallas import tpu as pltpu
from jax.sharding import PartitionSpec as P

BF = jnp.bfloat16
F32 = jnp.float32
UNIT = 4608
BLOCK = 128
MESH = pl.DeviceIdType.MESH
TOP = 80


def contract(left, right, left_dim, right_dim):
    return lax.dot_general(
        left, right, (((left_dim,), (right_dim,)), ((), ())), preferred_element_type=F32
    )


def gelu_pair(value):
    scale = 0.7978845608028654
    square = value * value
    inner = jnp.tanh(value * (scale + (scale * 0.044715) * square))
    half = 0.5 + 0.5 * inner
    act = value * half
    slope = half + (0.5 * value) * (1.0 - inner * inner) * (
        scale + (3.0 * 0.044715 * scale) * square
    )
    return act, slope


def layer_kernel(
    z_in,
    prefix_in,
    gate_hbm,
    up_hbm,
    down_hbm,
    acts_hbm,
    own_hbm,
    result,
    gate_w,
    up_w,
    down_w,
    xx,
    z_sib,
    levels,
    gate_f,
    up_f,
    back_f,
    acts,
    part,
    part_sib,
    line_two,
    line_four,
    block_half,
    block_one,
    fin,
    fin_sib,
    w_sem,
    z_sem,
    lev_sem,
    y_sem,
    one_sem,
    two_sem,
    sib_sem,
    send_sem,
    sib_send_sem,
    misc_send,
    rs_sem,
    act_sem,
    own_sem,
):
    toks = z_in.shape[2]
    rows = 2 * z_in.shape[1]
    y = lax.axis_index("dp")
    c = lax.axis_index("col")
    h = lax.rem(c, 2)
    chip = c // 2
    zc = chip // 4
    xc = lax.rem(chip, 4)
    o = 1 - h

    def at(d1, d2):
        zz = lax.rem(zc + (d1 % 4) * h + (d2 % 4) * o, 4)
        xq = lax.rem(xc + (d1 % 4) * o + (d2 % 4) * h, 4)
        return zz * 4 + xq

    def dev(d1, d2):
        return (y, at(d1, d2) * 2 + h)

    def row(d1, d2):
        return pl.multiple_of(at(d1, d2) * rows, 16)

    one_p, one_m = dev(1, 0), dev(-1, 0)
    two_p, two_m = dev(0, 1), dev(0, -1)
    sib = (y, chip * 2 + o)
    y_p, y_m = (lax.rem(y + 1, 4), c), (lax.rem(y + 3, 4), c)

    def blk(s, d1, d2, lo=0, n=None):
        start = row(d1, d2)
        return xx.at[h, s, pl.ds(start + lo, rows if n is None else n), :]

    def rput(src, dst, ssem, rsem, to):
        pltpu.make_async_remote_copy(
            src_ref=src, dst_ref=dst, send_sem=ssem, recv_sem=rsem, device_id=to, device_id_type=MESH
        ).start()

    def await_(ref, sem):
        pltpu.make_async_copy(ref, ref, sem).wait()

    loads = [
        pltpu.make_async_copy(src, dst, w_sem.at[k])
        for k, (src, dst) in enumerate(((gate_hbm, gate_w), (up_hbm, up_w), (down_hbm, down_w)))
    ]
    for load in loads:
        load.start()

    barrier = pltpu.get_barrier_semaphore()
    for to in (sib, one_p, one_m, two_p, two_m, y_p, y_m):
        pl.semaphore_signal(barrier, inc=1, device_id=to, device_id_type=MESH)
    pl.semaphore_wait(barrier, 7)

    rput(z_in, z_sib, misc_send.at[0], z_sem.at[0], sib)
    levels[0] = prefix_in[...]
    await_(z_sib, z_sem.at[0])
    mine, other = z_in[h].astype(F32), z_sib[h].astype(F32)
    low = jnp.where(h == 0, mine, other)
    high = jnp.where(h == 0, other, mine)
    xx[h, 0, pl.ds(row(0, 0), rows), :] = jnp.concatenate([low, high], axis=0).astype(BF)

    rest = rows - TOP
    offs = (0, -1, 1, 2)

    def to_sib(s, d1, d2):
        rput(blk(s, d1, d2), blk(s, d1, d2), sib_send_sem.at[s], sib_sem.at[s], sib)

    def across(s, i):
        d1 = offs[i]
        b = blk(s, d1, 0)
        rput(b, b, send_sem.at[s], two_sem.at[s, i], two_p)
        rput(b, b, send_sem.at[s], two_sem.at[s, 4 + i], two_m)

    def ev_a(s):
        if s in (1, 2):
            await_(blk(s, 0, 0), y_sem.at[s - 1])
        if s == 3:
            await_(blk(s, 0, 0, 0, TOP), y_sem.at[2])
            await_(blk(s, 0, 0, TOP, rest), y_sem.at[3])
        b = blk(s, 0, 0)
        rput(b, b, send_sem.at[s], one_sem.at[s, 0], one_p)
        rput(b, b, send_sem.at[s], one_sem.at[s, 1], one_m)
        across(s, 0)
        to_sib(s, 0, 0)

    def ev_b(s):
        await_(blk(s, -1, 0), one_sem.at[s, 0])
        b = blk(s, -1, 0, 0, TOP)
        rput(b, b, send_sem.at[s], one_sem.at[s, 2], one_p)
        await_(blk(s, 1, 0), one_sem.at[s, 1])
        b = blk(s, 1, 0, TOP, rest)
        rput(b, b, send_sem.at[s], one_sem.at[s, 3], one_m)
        across(s, 1)
        across(s, 2)
        to_sib(s, -1, 0)
        to_sib(s, 1, 0)

    def from_two(s, i):
        d1 = offs[i]
        await_(blk(s, d1, -1), two_sem.at[s, i])
        if i in (0, 2):
            b = blk(s, d1, -1)
            rput(b, b, send_sem.at[s], two_sem.at[s, 8 + i], two_p)
        to_sib(s, d1, -1)
        await_(blk(s, d1, 1), two_sem.at[s, 4 + i])
        if i in (1, 3):
            b = blk(s, d1, 1)
            rput(b, b, send_sem.at[s], two_sem.at[s, 8 + i], two_m)
        to_sib(s, d1, 1)

    def ev_c(s):
        from_two(s, 0)
        await_(blk(s, 2, 0, 0, TOP), one_sem.at[s, 2])
        await_(blk(s, 2, 0, TOP, rest), one_sem.at[s, 3])
        across(s, 3)
        to_sib(s, 2, 0)

    def ev_d(s):
        from_two(s, 1)
        from_two(s, 2)
        from_two(s, 3)

    def ev_e(s):
        for i in range(4):
            await_(blk(s, offs[i], 2), two_sem.at[s, 8 + i])
            to_sib(s, offs[i], 2)

    def ev_f(s):
        await_(xx.at[o, s], sib_sem.at[s])
        start = pl.multiple_of(y * (4 * rows), 16)
        for a in range(2):
            pltpu.make_async_copy(
                xx.at[a, s, pl.ds(start, 4 * rows), :],
                own_hbm.at[a, :, pl.ds(s * toks, toks)],
                own_sem.at[a, s],
            ).start()

    def y_send():
        b = blk(0, 0, 0)
        rput(b, blk(1, 0, 0), misc_send.at[1], y_sem.at[0], y_p)
        rput(b, blk(2, 0, 0), misc_send.at[1], y_sem.at[1], y_m)
        rput(prefix_in, levels.at[1], misc_send.at[2], lev_sem.at[0], y_p)
        rput(prefix_in, levels.at[2], misc_send.at[2], lev_sem.at[1], y_m)

    def y_forward():
        rput(blk(1, 0, 0, 0, TOP), blk(3, 0, 0, 0, TOP), misc_send.at[1], y_sem.at[2], y_p)
        rput(blk(2, 0, 0, TOP, rest), blk(3, 0, 0, TOP, rest), misc_send.at[1], y_sem.at[3], y_m)
        await_(levels.at[1], lev_sem.at[0])
        await_(levels.at[2], lev_sem.at[1])
        rput(levels.at[1], levels.at[3], misc_send.at[2], lev_sem.at[2], y_p)

    def gate_step(s):
        gate_f[...] = contract(xx[0, s], gate_w[...], 0, 0)

    def up_step(s):
        up_f[...] = contract(xx[0, s], up_w[...], 0, 0)

    def back_step(s):
        back_f[...] = contract(xx[1, s], down_w[...], 0, 1)

    def act_copy(s):
        return pltpu.make_async_copy(
            acts.at[s % 2], acts_hbm.at[:, pl.ds(s * toks, toks), :], act_sem.at[s]
        )

    def point_step(s):
        local = gate_w.shape[1]
        if s == 3:
            await_(levels.at[3], lev_sem.at[2])
        if s >= 2:
            act_copy(s - 2).wait()
        width = jnp.left_shift(jnp.full(levels.shape[1:], UNIT, jnp.int32), levels[s])
        mask = jnp.where(c * local < width, 1.0, 0.0).astype(F32)
        for b in range(toks // BLOCK):
            keep = jnp.broadcast_to(mask[b : b + 1, 0:1], (16, local))

            @pl.loop(0, BLOCK // 16)
            def _(k):
                r = pl.ds(pl.multiple_of(b * BLOCK + k * 16, 16), 16)
                act, slope = gelu_pair(gate_f[r, :])
                up = up_f[r, :] * keep
                back = back_f[r, :] * keep
                acts[s % 2, 2, r, :] = (act * up).astype(BF)
                acts[s % 2, 0, r, :] = (back * up * slope).astype(BF)
                acts[s % 2, 1, r, :] = (back * act).astype(BF)

        act_copy(s).start()

    third = xx.shape[2] // 3

    def out_step(t):
        part[0, pl.ds(t * third, third), :] = contract(
            down_w[:, pl.ds(t * third, third)], acts[0, 2], 0, 1
        ).astype(BF)

    def toward_step(t):
        r = pl.ds(t * third, third)
        part[1, r, :] = (
            contract(gate_w[r, :], acts[0, 0], 1, 1) + contract(up_w[r, :], acts[0, 1], 1, 1)
        ).astype(BF)

    def rs_0():
        rput(part.at[o], part_sib, misc_send.at[3], rs_sem.at[0], sib)

    def add_into(start, n, other):
        r = pl.ds(pl.multiple_of(start, 16), n)
        part[h, r, :] = (part[h, r, :].astype(F32) + other.astype(F32)).astype(BF)

    def pblk(d1, d2, lo=0, n=None):
        return part.at[h, pl.ds(row(d1, d2) + lo, rows if n is None else n), :]

    def rs_1():
        await_(part_sib, rs_sem.at[0])

        @pl.loop(0, 16)
        def _(k):
            start = k * rows
            add_into(start, rows, part_sib[pl.ds(pl.multiple_of(start, 16), rows), :])

        for j, i in enumerate((0, 2)):
            rput(pblk(offs[i], 2), line_two.at[0, j], misc_send.at[4], rs_sem.at[1 + j], two_p)
        for j, i in enumerate((1, 3)):
            rput(pblk(offs[i], 2), line_two.at[1, j], misc_send.at[4], rs_sem.at[3 + j], two_m)

    def rs_2():
        for j, i in enumerate((0, 2)):
            await_(line_two.at[0, j], rs_sem.at[1 + j])
            add_into(row(offs[i], 1), rows, line_two[0, j])
        for j, i in enumerate((1, 3)):
            await_(line_two.at[1, j], rs_sem.at[3 + j])
            add_into(row(offs[i], -1), rows, line_two[1, j])
        for i in range(4):
            rput(pblk(offs[i], 1), line_four.at[0, i], misc_send.at[5], rs_sem.at[5 + i], two_p)
            rput(pblk(offs[i], -1), line_four.at[1, i], misc_send.at[5], rs_sem.at[9 + i], two_m)

    def rs_3():
        for i in range(4):
            await_(line_four.at[0, i], rs_sem.at[5 + i])
            await_(line_four.at[1, i], rs_sem.at[9 + i])
            both = line_four[0, i].astype(F32) + line_four[1, i].astype(F32)
            add_into(row(offs[i], 0), rows, both)
        rput(
            pblk(2, 0, 0, TOP), block_half.at[pl.ds(0, TOP), :], misc_send.at[6], rs_sem.at[13], one_p
        )
        rput(
            pblk(2, 0, TOP, rest),
            block_half.at[pl.ds(TOP, rest), :],
            misc_send.at[6],
            rs_sem.at[14],
            one_m,
        )

    def rs_4():
        await_(block_half.at[pl.ds(0, TOP), :], rs_sem.at[13])
        add_into(row(1, 0), TOP, block_half[0:TOP, :])
        await_(block_half.at[pl.ds(TOP, rest), :], rs_sem.at[14])
        add_into(row(-1, 0) + TOP, rest, block_half[TOP:rows, :])
        rput(pblk(1, 0), block_one.at[0], misc_send.at[7], rs_sem.at[15], one_p)
        rput(pblk(-1, 0), block_one.at[1], misc_send.at[7], rs_sem.at[16], one_m)

    def rs_5():
        await_(block_one.at[0], rs_sem.at[15])
        await_(block_one.at[1], rs_sem.at[16])
        total = (
            part[h, pl.ds(row(0, 0), rows), :].astype(F32)
            + block_one[0].astype(F32)
            + block_one[1].astype(F32)
        )
        fin[0] = total[: rows // 2]
        fin[1] = total[rows // 2 :]
        rput(fin.at[o], fin_sib, misc_send.at[8], rs_sem.at[17], sib)

    def rs_6():
        await_(fin_sib, rs_sem.at[17])
        result[h] = fin[h]
        result[o] = fin_sib[...]

    ev_a(0)
    y_send()
    ev_b(0)
    ev_c(0)
    ev_d(0)
    ev_a(1)
    ev_a(2)
    y_forward()
    ev_e(0)
    ev_b(1)
    ev_f(0)
    loads[0].wait()
    gate_step(0)
    ev_c(1)
    loads[1].wait()
    up_step(0)
    ev_d(1)
    ev_b(2)
    loads[2].wait()
    back_step(0)
    ev_e(1)
    ev_c(2)
    point_step(0)
    ev_a(3)
    for t in range(3):
        out_step(t)
    ev_d(2)
    ev_b(3)
    for t in range(3):
        toward_step(t)
    ev_e(2)
    ev_c(3)
    rs_0()
    ev_f(1)
    gate_step(1)
    ev_d(3)
    rs_1()
    up_step(1)
    rs_2()
    back_step(1)
    ev_e(3)
    point_step(1)
    ev_f(2)
    gate_step(2)
    rs_3()
    up_step(2)
    rs_4()
    back_step(2)
    rs_5()
    point_step(2)
    ev_f(3)
    gate_step(3)
    rs_6()
    up_step(3)
    back_step(3)
    point_step(3)

    act_copy(2).wait()
    act_copy(3).wait()
    for s in range(4):
        for a in range(2):
            pltpu.make_async_copy(
                xx.at[a, s, pl.ds(0, 4 * rows), :],
                own_hbm.at[a, :, pl.ds(s * toks, toks)],
                own_sem.at[a, s],
            ).wait()
        await_(xx.at[0, s, pl.ds(0, 15 * rows), :], send_sem.at[s])
        await_(xx.at[0, s], sib_send_sem.at[s])
    await_(z_in, misc_send.at[0])
    await_(xx.at[0, 0, pl.ds(0, 3 * rows), :], misc_send.at[1])
    await_(levels.at[pl.ds(0, 3)], misc_send.at[2])
    await_(part_sib, misc_send.at[3])
    await_(line_two, misc_send.at[4])
    await_(line_four, misc_send.at[5])
    await_(block_half, misc_send.at[6])
    await_(block_one, misc_send.at[7])
    await_(fin_sib, misc_send.at[8])


def layer(z, levels, gate_weight, up_weight, down_weight):
    _, feats, toks = z.shape
    width, local = gate_weight.shape
    rows = 2 * feats
    dma = pltpu.SemaphoreType.DMA
    any_ = pl.BlockSpec(memory_space=pltpu.HBM)
    vmem = pl.BlockSpec(memory_space=pltpu.VMEM)
    return pl.pallas_call(
        layer_kernel,
        out_shape=(
            jax.ShapeDtypeStruct((3, 4 * toks, local), BF),
            jax.ShapeDtypeStruct((2, 4 * rows, 4 * toks), BF),
            jax.ShapeDtypeStruct((2, feats, toks), F32),
        ),
        in_specs=[vmem, vmem, any_, any_, any_],
        out_specs=(any_, any_, vmem),
        scratch_shapes=[
            pltpu.VMEM((width, local), BF),
            pltpu.VMEM((width, local), BF),
            pltpu.VMEM((local, width), BF),
            pltpu.VMEM((2, 4, width, toks), BF),
            pltpu.VMEM((2, feats, toks), BF),
            pltpu.VMEM((4, 8, 128), jnp.int32),
            pltpu.VMEM((toks, local), F32),
            pltpu.VMEM((toks, local), F32),
            pltpu.VMEM((toks, local), F32),
            pltpu.VMEM((2, 3, toks, local), BF),
            pltpu.VMEM((2, width, toks), BF),
            pltpu.VMEM((width, toks), BF),
            pltpu.VMEM((2, 2, rows, toks), BF),
            pltpu.VMEM((2, 4, rows, toks), BF),
            pltpu.VMEM((rows, toks), BF),
            pltpu.VMEM((2, rows, toks), BF),
            pltpu.VMEM((2, feats, toks), F32),
            pltpu.VMEM((feats, toks), F32),
            dma((3,)),
            dma((1,)),
            dma((3,)),
            dma((4,)),
            dma((4, 4)),
            dma((4, 12)),
            dma((4,)),
            dma((4,)),
            dma((4,)),
            dma((9,)),
            dma((18,)),
            dma((4,)),
            dma((2, 4)),
        ],
        compiler_params=pltpu.CompilerParams(
            collective_id=0, has_side_effects=True, vmem_limit_bytes=67043328
        ),
        name="layer",
    )(z, levels, gate_weight, up_weight, down_weight)


def grads_kernel(own, acts, gate_out, up_out, down_out):
    which = pl.program_id(0)
    value = jnp.dot(own[0], acts[0], preferred_element_type=F32)

    @pl.when(which == 0)
    def _():
        gate_out[...] = value.astype(BF)

    @pl.when(which == 1)
    def _():
        up_out[...] = value.astype(BF)

    @pl.when(which == 2)
    def _():
        down_out[...] = value.T.astype(BF)


def weight_grads(acts, own):
    _, toks, local = acts.shape
    feats = own.shape[1]
    tile = 384
    last = local // tile - 1
    return pl.pallas_call(
        grads_kernel,
        grid=(3, local // tile),
        out_shape=(
            jax.ShapeDtypeStruct((feats, local), BF),
            jax.ShapeDtypeStruct((feats, local), BF),
            jax.ShapeDtypeStruct((local, feats), BF),
        ),
        in_specs=[
            pl.BlockSpec((1, feats, toks), lambda a, n: (a // 2, 0, 0)),
            pl.BlockSpec((1, toks, tile), lambda a, n: (a, 0, n)),
        ],
        out_specs=(
            pl.BlockSpec((feats, tile), lambda a, n: (0, jnp.where(a == 0, n, last))),
            pl.BlockSpec((feats, tile), lambda a, n: (0, jnp.where(a == 1, n, jnp.where(a < 1, 0, last)))),
            pl.BlockSpec((tile, feats), lambda a, n: (jnp.where(a == 2, n, 0), 0)),
        ),
        compiler_params=pltpu.CompilerParams(vmem_limit_bytes=48 * 2**20),
        name="weight_grads",
    )(own, acts)


def body(tokens, cotangent, prefix, gate_weight, up_weight, down_weight):
    z = jnp.stack([tokens.T, cotangent.T])
    blocks = prefix.shape[0]
    levels = jnp.broadcast_to(jnp.pad(prefix, (0, 8 - blocks))[:, None], (8, 128))
    acts, own, result = layer(z, levels, gate_weight, up_weight, down_weight)
    grad_gate, grad_up, grad_down = weight_grads(acts, own)
    return (
        result[0].T.astype(BF),
        result[1].T.astype(BF),
        grad_gate,
        grad_up,
        grad_down,
    )


def solution(mesh):
    return jax.shard_map(
        body,
        mesh=mesh,
        in_specs=(
            P("dp", "col"),
            P("dp", "col"),
            P("dp"),
            P(None, "col"),
            P(None, "col"),
            P("col", None),
        ),
        out_specs=(P("dp", "col"), P("dp", "col"), P("dp", "col"), P("dp", "col"), P("col", "dp")),
        check_vma=False,
    )
```

```python
import functools

import jax
import jax.numpy as jnp
from jax import lax
from jax.experimental import pallas as pl
from jax.experimental.pallas import tpu as pltpu
from jax.sharding import PartitionSpec as P

BF = jnp.bfloat16
F32 = jnp.float32
UNIT = 4608
BLOCK = 128
MESH = pl.DeviceIdType.MESH
TOP = 80


def contract(left, right, left_dim, right_dim):
    return lax.dot_general(
        left, right, (((left_dim,), (right_dim,)), ((), ())), preferred_element_type=F32
    )


def gelu_pair(value):
    scale = 0.7978845608028654
    square = value * value
    inner = jnp.tanh(value * (scale + (scale * 0.044715) * square))
    half = 0.5 + 0.5 * inner
    act = value * half
    slope = half + (0.5 * value) * (1.0 - inner * inner) * (
        scale + (3.0 * 0.044715 * scale) * square
    )
    return act, slope


def layer_kernel(
    tokens_in,
    cotangent_in,
    prefix_in,
    gate_hbm,
    up_hbm,
    down_hbm,
    acts_hbm,
    own_hbm,
    out_ref,
    grad_ref,
    gate_w,
    up_w,
    down_w,
    xx,
    z_sib,
    levels,
    gate_f,
    up_f,
    back_f,
    acts,
    part,
    part_sib,
    line_two,
    line_four,
    block_half,
    block_one,
    fin,
    fin_sib,
    w_sem,
    z_sem,
    lev_sem,
    y_sem,
    one_sem,
    two_sem,
    sib_sem,
    send_sem,
    sib_send_sem,
    misc_send,
    rs_sem,
    act_sem,
    own_sem,
):
    feats, toks = tokens_in.shape
    rows = 2 * feats
    y = lax.axis_index("dp")
    c = lax.axis_index("col")
    h = lax.rem(c, 2)
    chip = c // 2
    zc = chip // 4
    xc = lax.rem(chip, 4)
    o = 1 - h

    def at(d1, d2):
        zz = lax.rem(zc + (d1 % 4) * h + (d2 % 4) * o, 4)
        xq = lax.rem(xc + (d1 % 4) * o + (d2 % 4) * h, 4)
        return zz * 4 + xq

    def dev(d1, d2):
        return (y, at(d1, d2) * 2 + h)

    def row(d1, d2):
        return pl.multiple_of(at(d1, d2) * rows, 16)

    one_p, one_m = dev(1, 0), dev(-1, 0)
    two_p, two_m = dev(0, 1), dev(0, -1)
    sib = (y, chip * 2 + o)
    y_p, y_m = (lax.rem(y + 1, 4), c), (lax.rem(y + 3, 4), c)

    def blk(s, d1, d2, lo=0, n=None):
        start = row(d1, d2)
        return xx.at[h, s, pl.ds(start + lo, rows if n is None else n), :]

    def rput(src, dst, ssem, rsem, to):
        pltpu.make_async_remote_copy(
            src_ref=src, dst_ref=dst, send_sem=ssem, recv_sem=rsem, device_id=to, device_id_type=MESH
        ).start()

    def await_(ref, sem):
        pltpu.make_async_copy(ref, ref, sem).wait()

    loads = [
        pltpu.make_async_copy(src, dst, w_sem.at[k])
        for k, (src, dst) in enumerate(((gate_hbm, gate_w), (up_hbm, up_w), (down_hbm, down_w)))
    ]
    for load in loads:
        load.start()

    barrier = pltpu.get_barrier_semaphore()
    for to in (sib, one_p, one_m, two_p, two_m, y_p, y_m):
        pl.semaphore_signal(barrier, inc=1, device_id=to, device_id_type=MESH)
    pl.semaphore_wait(barrier, 7)

    rput(tokens_in, z_sib.at[0], misc_send.at[0], z_sem.at[0], sib)
    rput(cotangent_in, z_sib.at[1], misc_send.at[0], z_sem.at[1], sib)
    which = lax.broadcasted_iota(jnp.int32, levels.shape[1:], 0)
    level = jnp.full(levels.shape[1:], prefix_in[0], jnp.int32)
    for b in range(1, prefix_in.shape[0]):
        level = jnp.where(which == b, prefix_in[b], level)
    levels[0] = level
    await_(z_sib.at[0], z_sem.at[0])
    await_(z_sib.at[1], z_sem.at[1])
    mine = jnp.where(h == 0, tokens_in[...].astype(F32), cotangent_in[...].astype(F32))
    other = z_sib[h].astype(F32)
    low = jnp.where(h == 0, mine, other)
    high = jnp.where(h == 0, other, mine)
    xx[h, 0, pl.ds(row(0, 0), rows), :] = jnp.concatenate([low, high], axis=0).astype(BF)

    rest = rows - TOP
    offs = (0, -1, 1, 2)

    def to_sib(s, d1, d2):
        b = blk(s, d1, d2)
        rput(b, b, sib_send_sem.at[s], sib_sem.at[s, d2 % 4], sib)

    def over_y(i, d1, d2):
        for slot, to in ((1, y_p), (2, y_m)):
            rput(
                blk(0, d1, d2), blk(slot, d1, d2), misc_send.at[9], two_sem.at[slot, i], to
            )

    def across(s, i):
        if s in (1, 2) and i == 3:
            return
        d1 = offs[i]
        b = blk(s, d1, 0)
        rput(b, b, send_sem.at[s], two_sem.at[s, i], two_p)
        rput(b, b, send_sem.at[s], two_sem.at[s, 4 + i], two_m)

    def ev_a(s):
        if s in (1, 2):
            await_(blk(s, 0, 0), y_sem.at[s - 1])
        if s == 3:
            await_(blk(s, 0, 0, 0, TOP), y_sem.at[2])
            await_(blk(s, 0, 0, TOP, rest), y_sem.at[3])
        b = blk(s, 0, 0)
        rput(b, b, send_sem.at[s], one_sem.at[s, 0], one_p)
        rput(b, b, send_sem.at[s], one_sem.at[s, 1], one_m)
        across(s, 0)
        to_sib(s, 0, 0)

    def ev_b1(s):
        await_(blk(s, -1, 0), one_sem.at[s, 0])
        b = blk(s, -1, 0, 0, TOP)
        rput(b, b, send_sem.at[s], one_sem.at[s, 2], one_p)
        across(s, 1)
        to_sib(s, -1, 0)

    def ev_b2(s):
        await_(blk(s, 1, 0), one_sem.at[s, 1])
        b = blk(s, 1, 0, TOP, rest)
        rput(b, b, send_sem.at[s], one_sem.at[s, 3], one_m)
        across(s, 2)
        to_sib(s, 1, 0)

    def ev_c(s):
        await_(blk(s, 2, 0, 0, TOP), one_sem.at[s, 2])
        await_(blk(s, 2, 0, TOP, rest), one_sem.at[s, 3])
        across(s, 3)
        to_sib(s, 2, 0)

    def ev_m(s, i):
        b = blk(s, offs[i], -1)
        await_(b, two_sem.at[s, i])
        if i in (0, 2) and s in (0, 3):
            rput(b, b, send_sem.at[s], two_sem.at[s, 8 + i], two_p)
        to_sib(s, offs[i], -1)
        if i == 3 and s == 0:
            over_y(i, offs[i], -1)

    def ev_p(s, i):
        b = blk(s, offs[i], 1)
        await_(b, two_sem.at[s, 4 + i])
        if i in (1, 3) and s in (0, 3):
            rput(b, b, send_sem.at[s], two_sem.at[s, 8 + i], two_m)
        to_sib(s, offs[i], 1)
        if i == 3 and s == 0:
            over_y(4 + i, offs[i], 1)

    def ev_e(s, i):
        await_(blk(s, offs[i], 2), two_sem.at[s, 8 + i])
        to_sib(s, offs[i], 2)
        if s == 0:
            over_y(8 + i, offs[i], 2)

    def await_line(s, k):
        await_(xx.at[o, s, pl.ds(0, 4 * rows), :], sib_sem.at[s, k])

    def chunk_step(k):
        d2 = (0, -1, 1, 2)[k]
        await_line(0, d2 % 4)
        r = pl.ds(pl.multiple_of(lax.rem(zc + d2 % 4, 4) * (4 * rows), 16), 4 * rows)
        gate = contract(xx[0, 0, r, :], gate_w[r, :], 0, 0)
        up = contract(xx[0, 0, r, :], up_w[r, :], 0, 0)
        if k == 0:
            gate_f[...] = gate
            up_f[...] = up
        else:
            gate_f[...] += gate
            up_f[...] += up

    def ev_f(s):
        if s > 0:
            for k in range(4):
                await_line(s, k)
        start = pl.multiple_of(y * (4 * rows), 16)
        for a in range(2):
            pltpu.make_async_copy(
                xx.at[a, s, pl.ds(start, 4 * rows), :],
                own_hbm.at[a, :, pl.ds(s * toks, toks)],
                own_sem.at[a, s],
            ).start()

    def y_send():
        b = blk(0, 0, 0)
        rput(b, blk(1, 0, 0), misc_send.at[1], y_sem.at[0], y_p)
        rput(b, blk(2, 0, 0), misc_send.at[1], y_sem.at[1], y_m)
        rput(levels.at[0], levels.at[1], misc_send.at[2], lev_sem.at[0], y_p)
        rput(levels.at[0], levels.at[2], misc_send.at[2], lev_sem.at[1], y_m)

    def y_forward():
        rput(blk(1, 0, 0, 0, TOP), blk(3, 0, 0, 0, TOP), misc_send.at[1], y_sem.at[2], y_p)
        rput(blk(2, 0, 0, TOP, rest), blk(3, 0, 0, TOP, rest), misc_send.at[1], y_sem.at[3], y_m)
        await_(levels.at[1], lev_sem.at[0])
        await_(levels.at[2], lev_sem.at[1])
        rput(levels.at[1], levels.at[3], misc_send.at[2], lev_sem.at[2], y_p)

    def gate_step(s):
        gate_f[...] = contract(xx[0, s], gate_w[...], 0, 0)

    def up_step(s):
        up_f[...] = contract(xx[0, s], up_w[...], 0, 0)

    def back_step(s):
        back_f[...] = contract(xx[1, s], down_w[...], 0, 1)

    def act_copy(s):
        return pltpu.make_async_copy(
            acts.at[s % 2], acts_hbm.at[:, pl.ds(s * toks, toks), :], act_sem.at[s]
        )

    def point_step(s, b):
        local = gate_w.shape[1]
        if s == 3 and b == 0:
            await_(levels.at[3], lev_sem.at[2])
        if s >= 2 and b == 0:
            act_copy(s - 2).wait()
        width = jnp.left_shift(jnp.full(levels.shape[1:], UNIT, jnp.int32), levels[s])
        mask = jnp.where(c * local < width, 1.0, 0.0).astype(F32)
        keep = jnp.broadcast_to(mask[b : b + 1, 0:1], (16, local))

        @pl.loop(0, BLOCK // 16)
        def _(k):
            r = pl.ds(pl.multiple_of(b * BLOCK + k * 16, 16), 16)
            act, slope = gelu_pair(gate_f[r, :])
            up = up_f[r, :] * keep
            back = back_f[r, :] * keep
            acts[s % 2, 2, r, :] = (act * up).astype(BF)
            acts[s % 2, 0, r, :] = (back * up * slope).astype(BF)
            acts[s % 2, 1, r, :] = (back * act).astype(BF)

        if b == toks // BLOCK - 1:
            act_copy(s).start()

    third = xx.shape[2] // 3

    def out_step(t):
        part[0, pl.ds(t * third, third), :] = contract(
            down_w[:, pl.ds(t * third, third)], acts[0, 2], 0, 1
        ).astype(BF)

    def toward_step(t):
        r = pl.ds(t * third, third)
        part[1, r, :] = (
            contract(gate_w[r, :], acts[0, 0], 1, 1) + contract(up_w[r, :], acts[0, 1], 1, 1)
        ).astype(BF)

    def rs_0():
        rput(part.at[o], part_sib, misc_send.at[3], rs_sem.at[0], sib)

    def add_into(start, n, other):
        r = pl.ds(pl.multiple_of(start, 16), n)
        part[h, r, :] = (part[h, r, :].astype(F32) + other.astype(F32)).astype(BF)

    def pblk(d1, d2, lo=0, n=None):
        return part.at[h, pl.ds(row(d1, d2) + lo, rows if n is None else n), :]

    def rs_1():
        await_(part_sib, rs_sem.at[0])

        @pl.loop(0, 16)
        def _(k):
            start = k * rows
            add_into(start, rows, part_sib[pl.ds(pl.multiple_of(start, 16), rows), :])

        for j, i in enumerate((0, 2)):
            rput(pblk(offs[i], 2), line_two.at[0, j], misc_send.at[4], rs_sem.at[1 + j], two_p)
        for j, i in enumerate((1, 3)):
            rput(pblk(offs[i], 2), line_two.at[1, j], misc_send.at[4], rs_sem.at[3 + j], two_m)

    def rs_2():
        for j, i in enumerate((0, 2)):
            await_(line_two.at[0, j], rs_sem.at[1 + j])
            add_into(row(offs[i], 1), rows, line_two[0, j])
        for j, i in enumerate((1, 3)):
            await_(line_two.at[1, j], rs_sem.at[3 + j])
            add_into(row(offs[i], -1), rows, line_two[1, j])
        for i in range(4):
            rput(pblk(offs[i], 1), line_four.at[0, i], misc_send.at[5], rs_sem.at[5 + i], two_p)
            rput(pblk(offs[i], -1), line_four.at[1, i], misc_send.at[5], rs_sem.at[9 + i], two_m)

    def rs_3():
        for i in range(4):
            await_(line_four.at[0, i], rs_sem.at[5 + i])
            await_(line_four.at[1, i], rs_sem.at[9 + i])
            both = line_four[0, i].astype(F32) + line_four[1, i].astype(F32)
            add_into(row(offs[i], 0), rows, both)
        rput(
            pblk(2, 0, 0, TOP), block_half.at[pl.ds(0, TOP), :], misc_send.at[6], rs_sem.at[13], one_p
        )
        rput(
            pblk(2, 0, TOP, rest),
            block_half.at[pl.ds(TOP, rest), :],
            misc_send.at[6],
            rs_sem.at[14],
            one_m,
        )

    def rs_4():
        await_(block_half.at[pl.ds(0, TOP), :], rs_sem.at[13])
        add_into(row(1, 0), TOP, block_half[0:TOP, :])
        await_(block_half.at[pl.ds(TOP, rest), :], rs_sem.at[14])
        add_into(row(-1, 0) + TOP, rest, block_half[TOP:rows, :])
        rput(pblk(1, 0), block_one.at[0], misc_send.at[7], rs_sem.at[15], one_p)
        rput(pblk(-1, 0), block_one.at[1], misc_send.at[7], rs_sem.at[16], one_m)

    def rs_5():
        await_(block_one.at[0], rs_sem.at[15])
        await_(block_one.at[1], rs_sem.at[16])
        total = (
            part[h, pl.ds(row(0, 0), rows), :].astype(F32)
            + block_one[0].astype(F32)
            + block_one[1].astype(F32)
        )
        fin[0] = total[: rows // 2]
        fin[1] = total[rows // 2 :]
        rput(fin.at[o], fin_sib, misc_send.at[8], rs_sem.at[17], sib)

    def rs_6():
        await_(fin_sib, rs_sem.at[17])
        mine, other = fin[h], fin_sib[...]
        out_ref[...] = jnp.where(h == 0, mine, other).astype(BF)
        grad_ref[...] = jnp.where(h == 0, other, mine).astype(BF)

    ev_a(0)
    y_send()
    ev_m(0, 0)
    ev_b2(0)
    ev_b1(0)
    ev_c(0)
    ev_p(0, 0)
    ev_p(0, 2)
    ev_e(0, 0)
    ev_p(0, 1)
    ev_m(0, 2)
    ev_p(0, 3)
    ev_a(1)
    ev_m(0, 1)
    ev_a(2)
    y_forward()
    loads[0].wait()
    loads[1].wait()
    chunk_step(0)
    ev_m(0, 3)
    chunk_step(1)
    ev_e(0, 2)
    ev_e(0, 3)
    ev_b2(1)
    ev_e(0, 1)
    chunk_step(2)
    chunk_step(3)
    ev_a(3)
    ev_b1(1)
    ev_f(0)
    loads[2].wait()
    back_step(0)
    ev_e(2, 0)
    point_step(0, 0)
    ev_p(2, 3)
    point_step(0, 1)
    point_step(0, 2)
    out_step(0)
    ev_m(1, 3)
    ev_p(1, 0)
    out_step(1)
    out_step(2)
    ev_b1(2)
    ev_b2(3)
    ev_b2(2)
    ev_p(1, 3)
    toward_step(0)
    ev_m(2, 3)
    ev_c(1)
    ev_e(1, 0)
    ev_b1(3)
    ev_m(2, 0)
    ev_p(1, 2)
    ev_e(2, 2)
    toward_step(1)
    ev_p(1, 1)
    ev_e(1, 2)
    ev_e(1, 3)
    ev_m(1, 2)
    ev_m(1, 0)
    ev_m(1, 1)
    toward_step(2)
    ev_e(1, 1)
    rs_0()
    ev_f(1)
    ev_c(3)
    gate_step(1)
    rs_1()
    ev_c(2)
    ev_p(3, 1)
    up_step(1)
    ev_e(2, 1)
    ev_p(2, 0)
    ev_p(2, 2)
    ev_m(2, 2)
    ev_m(2, 1)
    ev_m(3, 0)
    ev_m(3, 2)
    ev_p(2, 1)
    ev_p(3, 3)
    back_step(1)
    ev_e(2, 3)
    ev_m(3, 1)
    point_step(1, 0)
    point_step(1, 1)
    rs_2()
    ev_m(3, 3)
    point_step(1, 2)
    ev_f(2)
    gate_step(2)
    up_step(2)
    ev_e(3, 0)
    ev_e(3, 3)
    back_step(2)
    ev_e(3, 2)
    ev_e(3, 1)
    ev_p(3, 2)
    ev_p(3, 0)
    point_step(2, 0)
    point_step(2, 1)
    rs_3()
    point_step(2, 2)
    ev_f(3)
    gate_step(3)
    rs_4()
    up_step(3)
    back_step(3)
    rs_5()
    point_step(3, 0)
    point_step(3, 1)
    point_step(3, 2)
    rs_6()
    act_copy(2).wait()
    act_copy(3).wait()
    for s in range(4):
        for a in range(2):
            pltpu.make_async_copy(
                xx.at[a, s, pl.ds(0, 4 * rows), :],
                own_hbm.at[a, :, pl.ds(s * toks, toks)],
                own_sem.at[a, s],
            ).wait()
        sent = 15 if s in (0, 3) else 9
        await_(xx.at[0, s, pl.ds(0, sent * rows), :], send_sem.at[s])
        await_(xx.at[0, s], sib_send_sem.at[s])
    await_(z_sib, misc_send.at[0])
    await_(xx.at[0, 0, pl.ds(0, 3 * rows), :], misc_send.at[1])
    await_(levels.at[pl.ds(0, 3)], misc_send.at[2])
    await_(part_sib, misc_send.at[3])
    await_(line_two, misc_send.at[4])
    await_(line_four, misc_send.at[5])
    await_(block_half, misc_send.at[6])
    await_(block_one, misc_send.at[7])
    await_(fin_sib, misc_send.at[8])
    await_(xx.at[0, 0, pl.ds(0, 12 * rows), :], misc_send.at[9])


def layer(tokens, cotangent, prefix, gate_weight, up_weight, down_weight):
    feats, toks = tokens.shape
    width, local = gate_weight.shape
    rows = 2 * feats
    dma = pltpu.SemaphoreType.DMA
    any_ = pl.BlockSpec(memory_space=pltpu.HBM)
    vmem = pl.BlockSpec(memory_space=pltpu.VMEM)
    return pl.pallas_call(
        layer_kernel,
        out_shape=(
            jax.ShapeDtypeStruct((3, 4 * toks, local), BF),
            jax.ShapeDtypeStruct((2, 4 * rows, 4 * toks), BF),
            jax.ShapeDtypeStruct((feats, toks), BF),
            jax.ShapeDtypeStruct((feats, toks), BF),
        ),
        in_specs=[vmem, vmem, pl.BlockSpec(memory_space=pltpu.SMEM), any_, any_, any_],
        out_specs=(any_, any_, vmem, vmem),
        scratch_shapes=[
            pltpu.VMEM((width, local), BF),
            pltpu.VMEM((width, local), BF),
            pltpu.VMEM((local, width), BF),
            pltpu.VMEM((2, 4, width, toks), BF),
            pltpu.VMEM((2, feats, toks), BF),
            pltpu.VMEM((4, 8, 128), jnp.int32),
            pltpu.VMEM((toks, local), F32),
            pltpu.VMEM((toks, local), F32),
            pltpu.VMEM((toks, local), F32),
            pltpu.VMEM((2, 3, toks, local), BF),
            pltpu.VMEM((2, width, toks), BF),
            pltpu.VMEM((width, toks), BF),
            pltpu.VMEM((2, 2, rows, toks), BF),
            pltpu.VMEM((2, 4, rows, toks), BF),
            pltpu.VMEM((rows, toks), BF),
            pltpu.VMEM((2, rows, toks), BF),
            pltpu.VMEM((2, feats, toks), F32),
            pltpu.VMEM((feats, toks), F32),
            dma((3,)),
            dma((2,)),
            dma((3,)),
            dma((4,)),
            dma((4, 4)),
            dma((4, 12)),
            dma((4, 4)),
            dma((4,)),
            dma((4,)),
            dma((10,)),
            dma((18,)),
            dma((4,)),
            dma((2, 4)),
        ],
        compiler_params=pltpu.CompilerParams(
            collective_id=0, has_side_effects=True, vmem_limit_bytes=67043328
        ),
        name="layer",
    )(tokens, cotangent, prefix, gate_weight, up_weight, down_weight)


def grads_kernel(
    own_hbm,
    acts_hbm,
    first_hbm,
    second_hbm,
    gate_out,
    up_out,
    down_out,
    first_out,
    second_out,
    own,
    acts,
    done,
    small,
    in_sem,
    out_sem,
    small_sem,
):
    half = own.shape[2] // 2
    halves = (pl.ds(0, half), pl.ds(half, half))

    def own_load(a, j):
        return pltpu.make_async_copy(
            own_hbm.at[a, :, halves[j]], own.at[a, :, halves[j]], in_sem.at[2 * a + j]
        )

    def acts_load(k, j):
        return pltpu.make_async_copy(
            acts_hbm.at[k, halves[j]], acts.at[k, halves[j]], in_sem.at[4 + 2 * k + j]
        )

    for k in range(3):
        for j in range(2):
            if k != 1:
                own_load(k // 2, j).start()
            acts_load(k, j).start()
    brought = [
        pltpu.make_async_copy(src, small.at[j], small_sem.at[j])
        for j, src in enumerate((first_hbm, second_hbm))
    ]
    taken = [
        pltpu.make_async_copy(small.at[j], dst, small_sem.at[j])
        for j, dst in enumerate((first_out, second_out))
    ]
    for copy in brought:
        copy.start()
    outs = (gate_out, up_out, down_out)
    stores = [pltpu.make_async_copy(done.at[k], outs[k], out_sem.at[k]) for k in range(3)]

    @pl.loop(0, 3)
    def _(k):
        a = k // 2
        value = None
        for j in range(2):

            @pl.when(k != 1)
            def _():
                own_load(a, j).wait()

            acts_load(k, j).wait()
            term = jnp.dot(
                own[a, :, halves[j]], acts[k, halves[j], :], preferred_element_type=F32
            )
            value = term if value is None else value + term
        done[k] = value.astype(BF)
        for i in range(3):

            @pl.when(k == i)
            def _():
                stores[i].start()
                if i == 0:
                    for copy in brought:
                        copy.wait()
                    for copy in taken:
                        copy.start()

    for copy in stores + taken:
        copy.wait()


def weight_grads(acts, own, first, second):
    kinds, toks, local = acts.shape
    feats = own.shape[1]
    grad = jax.ShapeDtypeStruct((feats, local), BF)
    like = jax.ShapeDtypeStruct(first.shape, BF)
    hbm = pl.BlockSpec(memory_space=pltpu.HBM)
    return pl.pallas_call(
        grads_kernel,
        out_shape=(grad, grad, grad, like, like),
        in_specs=[hbm] * 4,
        out_specs=(hbm,) * 5,
        scratch_shapes=[
            pltpu.VMEM((2, feats, toks), BF),
            pltpu.VMEM((kinds, toks, local), BF),
            pltpu.VMEM((kinds, feats, local), BF),
            pltpu.VMEM((2, *first.shape), BF),
            pltpu.SemaphoreType.DMA((10,)),
            pltpu.SemaphoreType.DMA((3,)),
            pltpu.SemaphoreType.DMA((2,)),
        ],
        compiler_params=pltpu.CompilerParams(vmem_limit_bytes=67043328),
        name="weight_grads",
    )(own, acts, first, second)


def body(tokens, cotangent, prefix, gate_weight, up_weight, down_weight):
    acts, own, output, input_grad = layer(
        tokens.T, cotangent.T, prefix, gate_weight, up_weight, down_weight
    )
    grad_gate, grad_up, grad_down, output, input_grad = weight_grads(
        acts, own, output, input_grad
    )
    return output.T, input_grad.T, grad_gate, grad_up, grad_down.T


def solution(mesh):
    return jax.shard_map(
        body,
        mesh=mesh,
        in_specs=(
            P("dp", "col"),
            P("dp", "col"),
            P("dp"),
            P(None, "col"),
            P(None, "col"),
            P("col", None),
        ),
        out_specs=(P("dp", "col"), P("dp", "col"), P("dp", "col"), P("dp", "col"), P("col", "dp")),
        check_vma=False,
    )
```

```python
import functools

import jax
import jax.numpy as jnp
from jax import lax
from jax.experimental import pallas as pl
from jax.experimental.pallas import tpu as pltpu
from jax.sharding import PartitionSpec as P

BF = jnp.bfloat16
F32 = jnp.float32
UNIT = 4608
BLOCK = 128
MESH = pl.DeviceIdType.MESH
SHARED = 384
TOP = 80


def contract(left, right, left_dim, right_dim):
    return lax.dot_general(
        left, right, (((left_dim,), (right_dim,)), ((), ())), preferred_element_type=F32
    )


def gelu_pair(value):
    scale = 0.7978845608028654
    square = value * value
    inner = jnp.tanh(value * (scale + (scale * 0.044715) * square))
    half = 0.5 + 0.5 * inner
    act = value * half
    slope = half + (0.5 * value) * (1.0 - inner * inner) * (
        scale + (3.0 * 0.044715 * scale) * square
    )
    return act, slope


def layer_kernel(
    tokens_in,
    cotangent_in,
    prefix_in,
    gate_hbm,
    up_hbm,
    down_hbm,
    acts_hbm,
    own_hbm,
    out_ref,
    grad_ref,
    gate_w,
    up_w,
    down_w,
    xx,
    z_sib,
    levels,
    gate_f,
    up_f,
    acts,
    part,
    part_sib,
    line_two,
    line_four,
    block_half,
    block_one,
    fin,
    fin_sib,
    w_sem,
    z_sem,
    lev_sem,
    y_sem,
    one_sem,
    two_sem,
    sib_sem,
    send_sem,
    sib_send_sem,
    misc_send,
    rs_sem,
    act_sem,
    own_sem,
    share_sem,
):
    feats, toks = tokens_in.shape
    rows = 2 * feats
    y = lax.axis_index("dp")
    c = lax.axis_index("col")
    h = lax.rem(c, 2)
    chip = c // 2
    zc = chip // 4
    xc = lax.rem(chip, 4)
    o = 1 - h

    def at(d1, d2):
        zz = lax.rem(zc + (d1 % 4) * h + (d2 % 4) * o, 4)
        xq = lax.rem(xc + (d1 % 4) * o + (d2 % 4) * h, 4)
        return zz * 4 + xq

    def dev(d1, d2):
        return (y, at(d1, d2) * 2 + h)

    def row(d1, d2):
        return pl.multiple_of(at(d1, d2) * rows, 16)

    one_p, one_m = dev(1, 0), dev(-1, 0)
    two_p, two_m = dev(0, 1), dev(0, -1)
    sib = (y, chip * 2 + o)
    y_p, y_m = (lax.rem(y + 1, 4), c), (lax.rem(y + 3, 4), c)

    def blk(s, d1, d2, lo=0, n=None):
        start = row(d1, d2)
        return xx.at[h, s, pl.ds(start + lo, rows if n is None else n), :]

    def rput(src, dst, ssem, rsem, to):
        pltpu.make_async_remote_copy(
            src_ref=src, dst_ref=dst, send_sem=ssem, recv_sem=rsem, device_id=to, device_id_type=MESH
        ).start()

    def await_(ref, sem):
        pltpu.make_async_copy(ref, ref, sem).wait()

    loads = [
        pltpu.make_async_copy(src, dst, w_sem.at[k])
        for k, (src, dst) in enumerate(((gate_hbm, gate_w), (up_hbm, up_w), (down_hbm, down_w)))
    ]
    for load in loads:
        load.start()

    barrier = pltpu.get_barrier_semaphore()
    for to in (sib, one_p, one_m, two_p, two_m, y_p, y_m):
        pl.semaphore_signal(barrier, inc=1, device_id=to, device_id_type=MESH)
    pl.semaphore_wait(barrier, 7)

    rput(tokens_in, z_sib.at[0], misc_send.at[0], z_sem.at[0], sib)
    rput(cotangent_in, z_sib.at[1], misc_send.at[0], z_sem.at[1], sib)
    which = lax.broadcasted_iota(jnp.int32, levels.shape[1:], 0)
    level = jnp.full(levels.shape[1:], prefix_in[0], jnp.int32)
    for b in range(1, prefix_in.shape[0]):
        level = jnp.where(which == b, prefix_in[b], level)
    levels[0] = level
    await_(z_sib.at[0], z_sem.at[0])
    await_(z_sib.at[1], z_sem.at[1])
    mine = jnp.where(h == 0, tokens_in[...].astype(F32), cotangent_in[...].astype(F32))
    other = z_sib[h].astype(F32)
    low = jnp.where(h == 0, mine, other)
    high = jnp.where(h == 0, other, mine)
    xx[h, 0, pl.ds(row(0, 0), rows), :] = jnp.concatenate([low, high], axis=0).astype(BF)

    rest = rows - TOP
    offs = (0, -1, 1, 2)

    def to_sib(s, d1, d2):
        b = blk(s, d1, d2)
        rput(b, b, sib_send_sem.at[s], sib_sem.at[s, d2 % 4], sib)

    def over_y(i, d1, d2):
        for slot, to in ((1, y_p), (2, y_m)):
            rput(
                blk(0, d1, d2), blk(slot, d1, d2), misc_send.at[9], two_sem.at[slot, i], to
            )

    def across(s, i):
        if s in (1, 2) and i == 3:
            return
        d1 = offs[i]
        b = blk(s, d1, 0)
        rput(b, b, send_sem.at[s], two_sem.at[s, i], two_p)
        rput(b, b, send_sem.at[s], two_sem.at[s, 4 + i], two_m)

    def ev_a(s):
        if s in (1, 2):
            await_(blk(s, 0, 0), y_sem.at[s - 1])
        if s == 3:
            await_(blk(s, 0, 0, 0, TOP), y_sem.at[2])
            await_(blk(s, 0, 0, TOP, rest), y_sem.at[3])
        b = blk(s, 0, 0)
        rput(b, b, send_sem.at[s], one_sem.at[s, 0], one_p)
        rput(b, b, send_sem.at[s], one_sem.at[s, 1], one_m)
        across(s, 0)
        to_sib(s, 0, 0)

    def ev_b1(s):
        await_(blk(s, -1, 0), one_sem.at[s, 0])
        b = blk(s, -1, 0, 0, TOP)
        rput(b, b, send_sem.at[s], one_sem.at[s, 2], one_p)
        across(s, 1)
        to_sib(s, -1, 0)

    def ev_b2(s):
        await_(blk(s, 1, 0), one_sem.at[s, 1])
        b = blk(s, 1, 0, TOP, rest)
        rput(b, b, send_sem.at[s], one_sem.at[s, 3], one_m)
        across(s, 2)
        to_sib(s, 1, 0)

    def ev_c(s):
        await_(blk(s, 2, 0, 0, TOP), one_sem.at[s, 2])
        await_(blk(s, 2, 0, TOP, rest), one_sem.at[s, 3])
        across(s, 3)
        to_sib(s, 2, 0)

    def ev_m(s, i):
        b = blk(s, offs[i], -1)
        await_(b, two_sem.at[s, i])
        if i in (0, 2) and s in (0, 3):
            rput(b, b, send_sem.at[s], two_sem.at[s, 8 + i], two_p)
        to_sib(s, offs[i], -1)
        if i == 3 and s == 0:
            over_y(i, offs[i], -1)

    def ev_p(s, i):
        b = blk(s, offs[i], 1)
        await_(b, two_sem.at[s, 4 + i])
        if i in (1, 3) and s in (0, 3):
            rput(b, b, send_sem.at[s], two_sem.at[s, 8 + i], two_m)
        to_sib(s, offs[i], 1)
        if i == 3 and s == 0:
            over_y(4 + i, offs[i], 1)

    def ev_e(s, i):
        await_(blk(s, offs[i], 2), two_sem.at[s, 8 + i])
        to_sib(s, offs[i], 2)
        if s == 0:
            over_y(8 + i, offs[i], 2)

    def await_line(s, k):
        await_(xx.at[o, s, pl.ds(0, 4 * rows), :], sib_sem.at[s, k])

    def chunk_step(k):
        d2 = (0, -1, 1, 2)[k]
        await_line(0, d2 % 4)
        r = pl.ds(pl.multiple_of(lax.rem(zc + d2 % 4, 4) * (4 * rows), 16), 4 * rows)
        gate = contract(xx[0, 0, r, :], gate_w[r, :], 0, 0)
        up = contract(xx[0, 0, r, :], up_w[r, :], 0, 0)
        if k == 0:
            gate_f[...] = gate
            up_f[...] = up
        else:
            gate_f[...] += gate
            up_f[...] += up

    def ev_f(s):
        if s > 0:
            for k in range(4):
                await_line(s, k)
        start = pl.multiple_of(y * (4 * rows), 16)
        for a in range(2):
            pltpu.make_async_copy(
                xx.at[a, s, pl.ds(start, 4 * rows), :],
                own_hbm.at[a, :, pl.ds(s * toks, toks)],
                own_sem.at[a, s],
            ).start()

    def y_send():
        b = blk(0, 0, 0)
        rput(b, blk(1, 0, 0), misc_send.at[1], y_sem.at[0], y_p)
        rput(b, blk(2, 0, 0), misc_send.at[1], y_sem.at[1], y_m)
        rput(levels.at[0], levels.at[1], misc_send.at[2], lev_sem.at[0], y_p)
        rput(levels.at[0], levels.at[2], misc_send.at[2], lev_sem.at[1], y_m)

    def y_forward():
        rput(blk(1, 0, 0, 0, TOP), blk(3, 0, 0, 0, TOP), misc_send.at[1], y_sem.at[2], y_p)
        rput(blk(2, 0, 0, TOP, rest), blk(3, 0, 0, TOP, rest), misc_send.at[1], y_sem.at[3], y_m)
        await_(levels.at[1], lev_sem.at[0])
        await_(levels.at[2], lev_sem.at[1])
        rput(levels.at[1], levels.at[3], misc_send.at[2], lev_sem.at[2], y_p)

    local = gate_w.shape[1]
    kept = (local, local - SHARED, local - SHARED, local)

    def gate_step(s):
        gate_f[:, : kept[s]] = contract(xx[0, s], gate_w[:, : kept[s]], 0, 0)

    def up_step(s):
        up_f[:, : kept[s]] = contract(xx[0, s], up_w[:, : kept[s]], 0, 0)

    def act_copy(s):
        return pltpu.make_async_copy(
            acts.at[s % 2, :, :, pl.ds(0, kept[s])],
            acts_hbm.at[:, pl.ds(s * toks, toks), pl.ds(0, kept[s])],
            act_sem.at[s],
        )

    def shared(slot):
        return acts_hbm.at[:, pl.ds(slot * toks, toks), pl.ds(local - SHARED, SHARED)]

    def share_acts():
        act_copy(0).wait()
        rput(shared(0), shared(1), misc_send.at[10], share_sem.at[0], y_p)
        rput(shared(0), shared(2), misc_send.at[11], share_sem.at[1], y_m)

    def await_shared():
        await_(shared(1), share_sem.at[0])
        await_(shared(2), share_sem.at[1])

    def back_step(s):
        n = kept[s]
        if s == 3:
            await_(levels.at[3], lev_sem.at[2])
            act_copy(1).wait()
        width = jnp.left_shift(jnp.full(levels.shape[1:], UNIT, jnp.int32), levels[s])
        mask = jnp.where(c * local < width, 1.0, 0.0).astype(F32)
        back_all = contract(xx[1, s], down_w[:n, :], 0, 1)
        for b in range(toks // BLOCK):
            keep = jnp.broadcast_to(mask[b : b + 1, 0:1], (16, n))
            for k in range(BLOCK // 16):
                start = b * BLOCK + k * 16
                r = pl.ds(start, 16)
                act, slope = gelu_pair(gate_f[r, :n])
                up = up_f[r, :n] * keep
                back = back_all[start : start + 16] * keep
                acts[s % 2, 2, r, :n] = (act * up).astype(BF)
                acts[s % 2, 0, r, :n] = (back * up * slope).astype(BF)
                acts[s % 2, 1, r, :n] = (back * act).astype(BF)
        act_copy(s).start()

    third = xx.shape[2] // 3

    def out_step(t):
        part[0, pl.ds(t * third, third), :] = contract(
            acts[0, 2], down_w[:, pl.ds(t * third, third)], 1, 0
        ).T.astype(BF)

    def toward_step(t):
        r = pl.ds(t * third, third)
        part[1, r, :] = (
            contract(acts[0, 0], gate_w[r, :], 1, 1) + contract(acts[0, 1], up_w[r, :], 1, 1)
        ).T.astype(BF)

    def rs_0(t):
        r = pl.ds(t * third, third)
        rput(part.at[o, r, :], part_sib.at[r, :], misc_send.at[3], rs_sem.at[(0, 18, 19)[t]], sib)

    def add_into(start, n, other):
        r = pl.ds(pl.multiple_of(start, 16), n)
        part[h, r, :] = (part[h, r, :].astype(F32) + other.astype(F32)).astype(BF)

    def pblk(d1, d2, lo=0, n=None):
        return part.at[h, pl.ds(row(d1, d2) + lo, rows if n is None else n), :]

    def rs_1():
        for t in range(3):
            await_(part_sib.at[pl.ds(t * third, third), :], rs_sem.at[(0, 18, 19)[t]])

        @pl.loop(0, 16)
        def _(k):
            start = k * rows
            add_into(start, rows, part_sib[pl.ds(pl.multiple_of(start, 16), rows), :])

        for j, i in enumerate((0, 2)):
            rput(pblk(offs[i], 2), line_two.at[0, j], misc_send.at[4], rs_sem.at[1 + j], two_p)
        for j, i in enumerate((1, 3)):
            rput(pblk(offs[i], 2), line_two.at[1, j], misc_send.at[4], rs_sem.at[3 + j], two_m)

    def rs_2():
        for j, i in enumerate((0, 2)):
            await_(line_two.at[0, j], rs_sem.at[1 + j])
            add_into(row(offs[i], 1), rows, line_two[0, j])
        for j, i in enumerate((1, 3)):
            await_(line_two.at[1, j], rs_sem.at[3 + j])
            add_into(row(offs[i], -1), rows, line_two[1, j])
        for i in range(4):
            rput(pblk(offs[i], 1), line_four.at[0, i], misc_send.at[5], rs_sem.at[5 + i], two_p)
            rput(pblk(offs[i], -1), line_four.at[1, i], misc_send.at[5], rs_sem.at[9 + i], two_m)

    def rs_3():
        for i in range(4):
            await_(line_four.at[0, i], rs_sem.at[5 + i])
            await_(line_four.at[1, i], rs_sem.at[9 + i])
            both = line_four[0, i].astype(F32) + line_four[1, i].astype(F32)
            add_into(row(offs[i], 0), rows, both)
        rput(
            pblk(2, 0, 0, TOP), block_half.at[pl.ds(0, TOP), :], misc_send.at[6], rs_sem.at[13], one_p
        )
        rput(
            pblk(2, 0, TOP, rest),
            block_half.at[pl.ds(TOP, rest), :],
            misc_send.at[6],
            rs_sem.at[14],
            one_m,
        )

    def rs_4():
        await_(block_half.at[pl.ds(0, TOP), :], rs_sem.at[13])
        add_into(row(1, 0), TOP, block_half[0:TOP, :])
        await_(block_half.at[pl.ds(TOP, rest), :], rs_sem.at[14])
        add_into(row(-1, 0) + TOP, rest, block_half[TOP:rows, :])
        rput(pblk(1, 0), block_one.at[0], misc_send.at[7], rs_sem.at[15], one_p)
        rput(pblk(-1, 0), block_one.at[1], misc_send.at[7], rs_sem.at[16], one_m)

    def rs_5():
        await_(block_one.at[0], rs_sem.at[15])
        await_(block_one.at[1], rs_sem.at[16])
        total = (
            part[h, pl.ds(row(0, 0), rows), :].astype(F32)
            + block_one[0].astype(F32)
            + block_one[1].astype(F32)
        )
        fin[0] = total[: rows // 2]
        fin[1] = total[rows // 2 :]
        rput(fin.at[o], fin_sib, misc_send.at[8], rs_sem.at[17], sib)

    def rs_6():
        await_(fin_sib, rs_sem.at[17])
        mine, other = fin[h], fin_sib[...]
        out_ref[...] = jnp.where(h == 0, mine, other).astype(BF)
        grad_ref[...] = jnp.where(h == 0, other, mine).astype(BF)

    ev_a(0)
    y_send()
    ev_b2(0)
    ev_b1(0)
    ev_c(0)
    ev_m(0, 0)
    ev_m(0, 2)
    ev_p(0, 1)
    ev_m(0, 1)
    ev_p(0, 3)
    ev_a(1)
    ev_p(0, 0)
    ev_a(2)
    y_forward()
    ev_p(0, 2)
    loads[0].wait()
    loads[1].wait()
    chunk_step(0)
    ev_e(0, 0)
    ev_m(0, 3)
    chunk_step(1)
    ev_e(0, 2)
    ev_e(0, 3)
    ev_b1(1)
    ev_e(0, 1)
    chunk_step(2)
    chunk_step(3)
    ev_a(3)
    ev_f(0)
    ev_m(1, 0)
    ev_b2(1)
    ev_b1(2)
    ev_p(1, 0)
    ev_b2(2)
    loads[2].wait()
    back_step(0)
    ev_p(2, 3)
    ev_e(1, 0)
    out_step(0)
    out_step(1)
    share_acts()
    ev_b2(3)
    ev_m(1, 3)
    out_step(2)
    ev_m(1, 1)
    toward_step(0)
    rs_0(0)
    ev_b1(3)
    ev_p(1, 3)
    ev_p(1, 1)
    ev_c(1)
    toward_step(1)
    rs_0(1)
    ev_m(1, 2)
    ev_p(1, 2)
    ev_e(2, 0)
    ev_e(2, 2)
    ev_e(1, 2)
    toward_step(2)
    rs_0(2)
    ev_e(1, 1)
    ev_c(3)
    ev_e(1, 3)
    ev_p(2, 0)
    ev_e(2, 3)
    ev_m(2, 3)
    ev_f(1)
    gate_step(1)
    rs_1()
    ev_p(3, 1)
    ev_p(3, 0)
    ev_e(2, 1)
    ev_m(3, 2)
    ev_c(2)
    ev_m(2, 0)
    ev_p(2, 2)
    ev_m(2, 2)
    ev_m(2, 1)
    up_step(1)
    ev_m(3, 0)
    ev_p(3, 2)
    ev_m(3, 3)
    ev_p(3, 3)
    ev_p(2, 1)
    back_step(1)
    rs_2()
    ev_f(2)
    gate_step(2)
    up_step(2)
    ev_e(3, 0)
    ev_e(3, 2)
    ev_e(3, 3)
    ev_e(3, 1)
    ev_m(3, 1)
    back_step(2)
    rs_3()
    ev_f(3)
    gate_step(3)
    rs_4()
    up_step(3)
    rs_5()
    back_step(3)
    await_shared()
    rs_6()
    act_copy(2).wait()
    act_copy(3).wait()
    for s in range(4):
        for a in range(2):
            pltpu.make_async_copy(
                xx.at[a, s, pl.ds(0, 4 * rows), :],
                own_hbm.at[a, :, pl.ds(s * toks, toks)],
                own_sem.at[a, s],
            ).wait()
        sent = 15 if s in (0, 3) else 9
        await_(xx.at[0, s, pl.ds(0, sent * rows), :], send_sem.at[s])
        await_(xx.at[0, s], sib_send_sem.at[s])
    await_(z_sib, misc_send.at[0])
    await_(xx.at[0, 0, pl.ds(0, 3 * rows), :], misc_send.at[1])
    await_(levels.at[pl.ds(0, 3)], misc_send.at[2])
    await_(part_sib, misc_send.at[3])
    await_(line_two, misc_send.at[4])
    await_(line_four, misc_send.at[5])
    await_(block_half, misc_send.at[6])
    await_(block_one, misc_send.at[7])
    await_(fin_sib, misc_send.at[8])
    await_(xx.at[0, 0, pl.ds(0, 12 * rows), :], misc_send.at[9])
    await_(shared(0), misc_send.at[10])
    await_(shared(0), misc_send.at[11])


def layer(tokens, cotangent, prefix, gate_weight, up_weight, down_weight):
    feats, toks = tokens.shape
    width, local = gate_weight.shape
    rows = 2 * feats
    dma = pltpu.SemaphoreType.DMA
    any_ = pl.BlockSpec(memory_space=pltpu.HBM)
    vmem = pl.BlockSpec(memory_space=pltpu.VMEM)
    return pl.pallas_call(
        layer_kernel,
        out_shape=(
            jax.ShapeDtypeStruct((3, 4 * toks, local), BF),
            jax.ShapeDtypeStruct((2, 4 * rows, 4 * toks), BF),
            jax.ShapeDtypeStruct((feats, toks), BF),
            jax.ShapeDtypeStruct((feats, toks), BF),
        ),
        in_specs=[vmem, vmem, pl.BlockSpec(memory_space=pltpu.SMEM), any_, any_, any_],
        out_specs=(any_, any_, vmem, vmem),
        scratch_shapes=[
            pltpu.VMEM((width, local), BF),
            pltpu.VMEM((width, local), BF),
            pltpu.VMEM((local, width), BF),
            pltpu.VMEM((2, 4, width, toks), BF),
            pltpu.VMEM((2, feats, toks), BF),
            pltpu.VMEM((4, 8, 128), jnp.int32),
            pltpu.VMEM((toks, local), F32),
            pltpu.VMEM((toks, local), F32),
            pltpu.VMEM((2, 3, toks, local), BF),
            pltpu.VMEM((2, width, toks), BF),
            pltpu.VMEM((width, toks), BF),
            pltpu.VMEM((2, 2, rows, toks), BF),
            pltpu.VMEM((2, 4, rows, toks), BF),
            pltpu.VMEM((rows, toks), BF),
            pltpu.VMEM((2, rows, toks), BF),
            pltpu.VMEM((2, feats, toks), F32),
            pltpu.VMEM((feats, toks), F32),
            dma((3,)),
            dma((2,)),
            dma((3,)),
            dma((4,)),
            dma((4, 4)),
            dma((4, 12)),
            dma((4, 4)),
            dma((4,)),
            dma((4,)),
            dma((12,)),
            dma((20,)),
            dma((4,)),
            dma((2, 4)),
            dma((2,)),
        ],
        compiler_params=pltpu.CompilerParams(
            collective_id=0, has_side_effects=True, vmem_limit_bytes=67043328
        ),
        name="layer",
    )(tokens, cotangent, prefix, gate_weight, up_weight, down_weight)


def grads_kernel(
    own_hbm,
    acts_hbm,
    first_hbm,
    second_hbm,
    gate_out,
    up_out,
    down_out,
    first_out,
    second_out,
    own,
    acts,
    done,
    small,
    in_sem,
    out_sem,
    small_sem,
):
    half = own.shape[2] // 2
    halves = (pl.ds(0, half), pl.ds(half, half))

    def own_load(a, j):
        return pltpu.make_async_copy(
            own_hbm.at[a, :, halves[j]], own.at[a, :, halves[j]], in_sem.at[2 * a + j]
        )

    def acts_load(k, j):
        return pltpu.make_async_copy(
            acts_hbm.at[k, halves[j]], acts.at[k, halves[j]], in_sem.at[4 + 2 * k + j]
        )

    for j in range(2):
        own_load(0, j).start()
        acts_load(0, j).start()
    brought = [
        pltpu.make_async_copy(src, small.at[j], small_sem.at[j])
        for j, src in enumerate((first_hbm, second_hbm))
    ]
    taken = [
        pltpu.make_async_copy(small.at[j], dst, small_sem.at[j])
        for j, dst in enumerate((first_out, second_out))
    ]
    for copy in brought:
        copy.start()
    outs = (gate_out, up_out, down_out)
    stores = [pltpu.make_async_copy(done.at[k], outs[k], out_sem.at[k]) for k in range(3)]

    @pl.loop(0, 3)
    def _(k):
        a = k // 2
        value = None
        for j in range(2):

            @pl.when(k != 1)
            def _():
                own_load(a, j).wait()

            acts_load(k, j).wait()
            if j == 0:

                @pl.when(k == 1)
                def _():
                    own_load(1, 0).start()
                    own_load(1, 1).start()

                @pl.when(k < 2)
                def _():
                    acts_load(k + 1, 0).start()
                    acts_load(k + 1, 1).start()

            term = jnp.dot(
                own[a, :, halves[j]], acts[k, halves[j], :], preferred_element_type=F32
            )
            value = term if value is None else value + term
        done[k] = value.astype(BF)
        for i in range(3):

            @pl.when(k == i)
            def _():
                stores[i].start()
                if i == 0:
                    for copy in brought:
                        copy.wait()
                    for copy in taken:
                        copy.start()

    for copy in stores + taken:
        copy.wait()


def weight_grads(acts, own, first, second):
    kinds, toks, local = acts.shape
    feats = own.shape[1]
    grad = jax.ShapeDtypeStruct((feats, local), BF)
    like = jax.ShapeDtypeStruct(first.shape, BF)
    hbm = pl.BlockSpec(memory_space=pltpu.HBM)
    return pl.pallas_call(
        grads_kernel,
        out_shape=(grad, grad, grad, like, like),
        in_specs=[hbm] * 4,
        out_specs=(hbm,) * 5,
        scratch_shapes=[
            pltpu.VMEM((2, feats, toks), BF),
            pltpu.VMEM((kinds, toks, local), BF),
            pltpu.VMEM((kinds, feats, local), BF),
            pltpu.VMEM((2, *first.shape), BF),
            pltpu.SemaphoreType.DMA((10,)),
            pltpu.SemaphoreType.DMA((3,)),
            pltpu.SemaphoreType.DMA((2,)),
        ],
        compiler_params=pltpu.CompilerParams(vmem_limit_bytes=67043328),
        name="weight_grads",
    )(own, acts, first, second)


def body(tokens, cotangent, prefix, gate_weight, up_weight, down_weight):
    acts, own, output, input_grad = layer(
        tokens.T, cotangent.T, prefix, gate_weight, up_weight, down_weight
    )
    grad_gate, grad_up, grad_down, output, input_grad = weight_grads(
        acts, own, output, input_grad
    )
    return output.T, input_grad.T, grad_gate, grad_up, grad_down.T


def solution(mesh):
    return jax.shard_map(
        body,
        mesh=mesh,
        in_specs=(
            P("dp", "col"),
            P("dp", "col"),
            P("dp"),
            P(None, "col"),
            P(None, "col"),
            P("col", None),
        ),
        out_specs=(P("dp", "col"), P("dp", "col"), P("dp", "col"), P("dp", "col"), P("col", "dp")),
        check_vma=False,
    )
```

```python
import functools

import jax
import jax.numpy as jnp
from jax import lax
from jax.experimental import pallas as pl
from jax.experimental.pallas import tpu as pltpu
from jax.sharding import PartitionSpec as P

BF = jnp.bfloat16
F32 = jnp.float32
UNIT = 4608
BLOCK = 128
MESH = pl.DeviceIdType.MESH
SHARED = 384
TOP = 80


def contract(left, right, left_dim, right_dim):
    return lax.dot_general(
        left, right, (((left_dim,), (right_dim,)), ((), ())), preferred_element_type=F32
    )


def gelu_pair(value):
    scale = 0.7978845608028654
    square = value * value
    inner = jnp.tanh(value * (scale + (scale * 0.044715) * square))
    half = 0.5 + 0.5 * inner
    act = value * half
    slope = half + (0.5 * value) * (1.0 - inner * inner) * (
        scale + (3.0 * 0.044715 * scale) * square
    )
    return act, slope


def layer_kernel(
    tokens_in,
    cotangent_in,
    prefix_in,
    gate_hbm,
    up_hbm,
    down_hbm,
    acts_hbm,
    own_hbm,
    out_ref,
    grad_ref,
    gate_w,
    up_w,
    down_w,
    xx,
    z_sib,
    levels,
    gate_f,
    up_f,
    acts,
    part,
    part_sib,
    line_two,
    line_four,
    block_half,
    block_one,
    fin,
    fin_sib,
    w_sem,
    z_sem,
    lev_sem,
    y_sem,
    one_sem,
    two_sem,
    sib_sem,
    send_sem,
    sib_send_sem,
    misc_send,
    rs_sem,
    act_sem,
    own_sem,
    share_sem,
):
    feats, toks = tokens_in.shape
    rows = 2 * feats
    y = lax.axis_index("dp")
    c = lax.axis_index("col")
    h = lax.rem(c, 2)
    chip = c // 2
    zc = chip // 4
    xc = lax.rem(chip, 4)
    o = 1 - h

    def at(d1, d2):
        zz = lax.rem(zc + (d1 % 4) * h + (d2 % 4) * o, 4)
        xq = lax.rem(xc + (d1 % 4) * o + (d2 % 4) * h, 4)
        return zz * 4 + xq

    def dev(d1, d2):
        return (y, at(d1, d2) * 2 + h)

    def row(d1, d2):
        return pl.multiple_of(at(d1, d2) * rows, 16)

    one_p, one_m = dev(1, 0), dev(-1, 0)
    two_p, two_m = dev(0, 1), dev(0, -1)
    sib = (y, chip * 2 + o)
    y_p, y_m = (lax.rem(y + 1, 4), c), (lax.rem(y + 3, 4), c)

    def blk(s, d1, d2, lo=0, n=None):
        start = row(d1, d2)
        return xx.at[h, s, pl.ds(start + lo, rows if n is None else n), :]

    def rput(src, dst, ssem, rsem, to):
        pltpu.make_async_remote_copy(
            src_ref=src, dst_ref=dst, send_sem=ssem, recv_sem=rsem, device_id=to, device_id_type=MESH
        ).start()

    def await_(ref, sem):
        pltpu.make_async_copy(ref, ref, sem).wait()

    loads = [
        pltpu.make_async_copy(src, dst, w_sem.at[k])
        for k, (src, dst) in enumerate(((gate_hbm, gate_w), (up_hbm, up_w), (down_hbm, down_w)))
    ]
    for load in loads:
        load.start()

    barrier = pltpu.get_barrier_semaphore()
    for to in (sib, one_p, one_m, two_p, two_m, y_p, y_m):
        pl.semaphore_signal(barrier, inc=1, device_id=to, device_id_type=MESH)
    pl.semaphore_wait(barrier, 7)

    rput(tokens_in, z_sib.at[0], misc_send.at[0], z_sem.at[0], sib)
    rput(cotangent_in, z_sib.at[1], misc_send.at[0], z_sem.at[1], sib)
    which = lax.broadcasted_iota(jnp.int32, levels.shape[1:], 0)
    level = jnp.full(levels.shape[1:], prefix_in[0], jnp.int32)
    for b in range(1, prefix_in.shape[0]):
        level = jnp.where(which == b, prefix_in[b], level)
    levels[0] = level
    await_(z_sib.at[0], z_sem.at[0])
    await_(z_sib.at[1], z_sem.at[1])
    mine = jnp.where(h == 0, tokens_in[...].astype(F32), cotangent_in[...].astype(F32))
    other = z_sib[h].astype(F32)
    low = jnp.where(h == 0, mine, other)
    high = jnp.where(h == 0, other, mine)
    xx[h, 0, pl.ds(row(0, 0), rows), :] = jnp.concatenate([low, high], axis=0).astype(BF)

    rest = rows - TOP
    offs = (0, -1, 1, 2)

    def to_sib(s, d1, d2):
        b = blk(s, d1, d2)
        rput(b, b, sib_send_sem.at[s], sib_sem.at[s, d2 % 4], sib)

    def over_y(i, d1, d2):
        for slot, to in ((1, y_p), (2, y_m)):
            rput(
                blk(0, d1, d2), blk(slot, d1, d2), misc_send.at[9], two_sem.at[slot, i], to
            )

    def across(s, i):
        if s in (1, 2) and i == 3:
            return
        d1 = offs[i]
        b = blk(s, d1, 0)
        rput(b, b, send_sem.at[s], two_sem.at[s, i], two_p)
        rput(b, b, send_sem.at[s], two_sem.at[s, 4 + i], two_m)

    def ev_a(s):
        if s in (1, 2):
            await_(blk(s, 0, 0), y_sem.at[s - 1])
        if s == 3:
            await_(blk(s, 0, 0, 0, TOP), y_sem.at[2])
            await_(blk(s, 0, 0, TOP, rest), y_sem.at[3])
        b = blk(s, 0, 0)
        rput(b, b, send_sem.at[s], one_sem.at[s, 0], one_p)
        rput(b, b, send_sem.at[s], one_sem.at[s, 1], one_m)
        across(s, 0)
        to_sib(s, 0, 0)

    def ev_b1(s):
        await_(blk(s, -1, 0), one_sem.at[s, 0])
        b = blk(s, -1, 0, 0, TOP)
        rput(b, b, send_sem.at[s], one_sem.at[s, 2], one_p)
        across(s, 1)
        to_sib(s, -1, 0)

    def ev_b2(s):
        await_(blk(s, 1, 0), one_sem.at[s, 1])
        b = blk(s, 1, 0, TOP, rest)
        rput(b, b, send_sem.at[s], one_sem.at[s, 3], one_m)
        across(s, 2)
        to_sib(s, 1, 0)

    def ev_c(s):
        await_(blk(s, 2, 0, 0, TOP), one_sem.at[s, 2])
        await_(blk(s, 2, 0, TOP, rest), one_sem.at[s, 3])
        across(s, 3)
        to_sib(s, 2, 0)

    def ev_m(s, i):
        b = blk(s, offs[i], -1)
        await_(b, two_sem.at[s, i])
        if i in (0, 2) and s in (0, 3):
            rput(b, b, send_sem.at[s], two_sem.at[s, 8 + i], two_p)
        to_sib(s, offs[i], -1)
        if i == 3 and s == 0:
            over_y(i, offs[i], -1)

    def ev_p(s, i):
        b = blk(s, offs[i], 1)
        await_(b, two_sem.at[s, 4 + i])
        if i in (1, 3) and s in (0, 3):
            rput(b, b, send_sem.at[s], two_sem.at[s, 8 + i], two_m)
        to_sib(s, offs[i], 1)
        if i == 3 and s == 0:
            over_y(4 + i, offs[i], 1)

    def ev_e(s, i):
        await_(blk(s, offs[i], 2), two_sem.at[s, 8 + i])
        to_sib(s, offs[i], 2)
        if s == 0:
            over_y(8 + i, offs[i], 2)

    def await_line(s, k):
        await_(xx.at[o, s, pl.ds(0, 4 * rows), :], sib_sem.at[s, k])

    def chunk_step(k):
        d2 = (0, -1, 1, 2)[k]
        await_line(0, d2 % 4)
        r = pl.ds(pl.multiple_of(lax.rem(zc + d2 % 4, 4) * (4 * rows), 16), 4 * rows)
        gate = contract(xx[0, 0, r, :], gate_w[r, :], 0, 0)
        up = contract(xx[0, 0, r, :], up_w[r, :], 0, 0)
        if k == 0:
            gate_f[...] = gate
            up_f[...] = up
        else:
            gate_f[...] += gate
            up_f[...] += up

    def ev_f(s):
        if s > 0:
            for k in range(4):
                await_line(s, k)
        start = pl.multiple_of(y * (4 * rows), 16)
        for a in range(2):
            pltpu.make_async_copy(
                xx.at[a, s, pl.ds(start, 4 * rows), :],
                own_hbm.at[a, :, pl.ds(s * toks, toks)],
                own_sem.at[a, s],
            ).start()

    def y_send():
        b = blk(0, 0, 0)
        rput(b, blk(1, 0, 0), misc_send.at[1], y_sem.at[0], y_p)
        rput(b, blk(2, 0, 0), misc_send.at[1], y_sem.at[1], y_m)
        rput(levels.at[0], levels.at[1], misc_send.at[2], lev_sem.at[0], y_p)
        rput(levels.at[0], levels.at[2], misc_send.at[2], lev_sem.at[1], y_m)

    def y_forward():
        rput(blk(1, 0, 0, 0, TOP), blk(3, 0, 0, 0, TOP), misc_send.at[1], y_sem.at[2], y_p)
        rput(blk(2, 0, 0, TOP, rest), blk(3, 0, 0, TOP, rest), misc_send.at[1], y_sem.at[3], y_m)
        await_(levels.at[1], lev_sem.at[0])
        await_(levels.at[2], lev_sem.at[1])
        rput(levels.at[1], levels.at[3], misc_send.at[2], lev_sem.at[2], y_p)

    local = gate_w.shape[1]
    kept = (local, local - SHARED, local - SHARED, local)

    def gate_step(s):
        gate_f[:, : kept[s]] = contract(xx[0, s], gate_w[:, : kept[s]], 0, 0)

    def up_step(s):
        up_f[:, : kept[s]] = contract(xx[0, s], up_w[:, : kept[s]], 0, 0)

    def act_copy(s):
        return pltpu.make_async_copy(
            acts.at[s % 2, :, :, pl.ds(0, kept[s])],
            acts_hbm.at[:, pl.ds(s * toks, toks), pl.ds(0, kept[s])],
            act_sem.at[s],
        )

    def shared(slot):
        return acts_hbm.at[:, pl.ds(slot * toks, toks), pl.ds(local - SHARED, SHARED)]

    def share_acts():
        act_copy(0).wait()
        rput(shared(0), shared(1), misc_send.at[10], share_sem.at[0], y_p)
        rput(shared(0), shared(2), misc_send.at[11], share_sem.at[1], y_m)

    def await_shared():
        await_(shared(1), share_sem.at[0])
        await_(shared(2), share_sem.at[1])

    def back_step(s):
        n = kept[s]
        if s == 3:
            await_(levels.at[3], lev_sem.at[2])
            act_copy(1).wait()
        width = jnp.left_shift(jnp.full(levels.shape[1:], UNIT, jnp.int32), levels[s])
        mask = jnp.where(c * local < width, 1.0, 0.0).astype(F32)
        back_all = contract(xx[1, s], down_w[:n, :], 0, 1)
        for b in range(toks // BLOCK):
            keep = jnp.broadcast_to(mask[b : b + 1, 0:1], (16, n))
            for k in range(BLOCK // 16):
                start = b * BLOCK + k * 16
                r = pl.ds(start, 16)
                act, slope = gelu_pair(gate_f[r, :n])
                up = up_f[r, :n] * keep
                back = back_all[start : start + 16] * keep
                acts[s % 2, 2, r, :n] = (act * up).astype(BF)
                acts[s % 2, 0, r, :n] = (back * up * slope).astype(BF)
                acts[s % 2, 1, r, :n] = (back * act).astype(BF)
        act_copy(s).start()

    third = xx.shape[2] // 3

    def out_step(t):
        part[0, pl.ds(t * third, third), :] = contract(
            acts[0, 2], down_w[:, pl.ds(t * third, third)], 1, 0
        ).T.astype(BF)

    def toward_step(t):
        r = pl.ds(t * third, third)
        part[1, r, :] = (
            contract(acts[0, 0], gate_w[r, :], 1, 1) + contract(acts[0, 1], up_w[r, :], 1, 1)
        ).T.astype(BF)

    def rs_0(t):
        r = pl.ds(t * third, third)
        rput(part.at[o, r, :], part_sib.at[r, :], misc_send.at[3], rs_sem.at[(0, 18, 19)[t]], sib)

    def add_into(start, n, other):
        r = pl.ds(pl.multiple_of(start, 16), n)
        part[h, r, :] = (part[h, r, :].astype(F32) + other.astype(F32)).astype(BF)

    def pblk(d1, d2, lo=0, n=None):
        return part.at[h, pl.ds(row(d1, d2) + lo, rows if n is None else n), :]

    def rs_1():
        for t in range(3):
            await_(part_sib.at[pl.ds(t * third, third), :], rs_sem.at[(0, 18, 19)[t]])

        @pl.loop(0, 16)
        def _(k):
            start = k * rows
            add_into(start, rows, part_sib[pl.ds(pl.multiple_of(start, 16), rows), :])

        for j, i in enumerate((0, 2)):
            rput(pblk(offs[i], 2), line_two.at[0, j], misc_send.at[4], rs_sem.at[1 + j], two_p)
        for j, i in enumerate((1, 3)):
            rput(pblk(offs[i], 2), line_two.at[1, j], misc_send.at[4], rs_sem.at[3 + j], two_m)

    def rs_2():
        for j, i in enumerate((0, 2)):
            await_(line_two.at[0, j], rs_sem.at[1 + j])
            add_into(row(offs[i], 1), rows, line_two[0, j])
        for j, i in enumerate((1, 3)):
            await_(line_two.at[1, j], rs_sem.at[3 + j])
            add_into(row(offs[i], -1), rows, line_two[1, j])
        for i in range(4):
            rput(pblk(offs[i], 1), line_four.at[0, i], misc_send.at[5], rs_sem.at[5 + i], two_p)
            rput(pblk(offs[i], -1), line_four.at[1, i], misc_send.at[5], rs_sem.at[9 + i], two_m)

    def rs_3():
        for i in range(4):
            await_(line_four.at[0, i], rs_sem.at[5 + i])
            await_(line_four.at[1, i], rs_sem.at[9 + i])
            both = line_four[0, i].astype(F32) + line_four[1, i].astype(F32)
            add_into(row(offs[i], 0), rows, both)
        rput(
            pblk(2, 0, 0, TOP), block_half.at[pl.ds(0, TOP), :], misc_send.at[6], rs_sem.at[13], one_p
        )
        rput(
            pblk(2, 0, TOP, rest),
            block_half.at[pl.ds(TOP, rest), :],
            misc_send.at[6],
            rs_sem.at[14],
            one_m,
        )

    def rs_4():
        await_(block_half.at[pl.ds(0, TOP), :], rs_sem.at[13])
        add_into(row(1, 0), TOP, block_half[0:TOP, :])
        await_(block_half.at[pl.ds(TOP, rest), :], rs_sem.at[14])
        add_into(row(-1, 0) + TOP, rest, block_half[TOP:rows, :])
        rput(pblk(1, 0), block_one.at[0], misc_send.at[7], rs_sem.at[15], one_p)
        rput(pblk(-1, 0), block_one.at[1], misc_send.at[7], rs_sem.at[16], one_m)

    def rs_5():
        await_(block_one.at[0], rs_sem.at[15])
        await_(block_one.at[1], rs_sem.at[16])
        total = (
            part[h, pl.ds(row(0, 0), rows), :].astype(F32)
            + block_one[0].astype(F32)
            + block_one[1].astype(F32)
        )
        fin[0] = total[: rows // 2]
        fin[1] = total[rows // 2 :]
        rput(fin.at[o], fin_sib, misc_send.at[8], rs_sem.at[17], sib)

    def rs_6():
        await_(fin_sib, rs_sem.at[17])
        mine, other = fin[h], fin_sib[...]
        out_ref[...] = jnp.where(h == 0, mine, other).astype(BF)
        grad_ref[...] = jnp.where(h == 0, other, mine).astype(BF)

    ev_a(0)
    ev_m(0, 0)
    ev_b2(0)
    y_send()
    ev_b1(0)
    ev_c(0)
    ev_p(0, 0)
    ev_e(0, 0)
    ev_p(0, 1)
    ev_m(0, 2)
    ev_p(0, 3)
    ev_m(0, 1)
    ev_a(1)
    ev_a(2)
    y_forward()
    loads[0].wait()
    loads[1].wait()
    chunk_step(0)
    ev_m(0, 3)
    ev_e(0, 1)
    ev_p(0, 2)
    chunk_step(1)
    ev_e(0, 2)
    ev_e(0, 3)
    chunk_step(2)
    ev_b1(1)
    ev_e(2, 0)
    ev_b2(1)
    chunk_step(3)
    ev_f(0)
    ev_a(3)
    loads[2].wait()
    back_step(0)
    ev_p(1, 3)
    out_step(0)
    ev_b1(2)
    ev_b2(2)
    ev_m(1, 3)
    out_step(1)
    ev_m(1, 0)
    share_acts()
    ev_p(1, 0)
    out_step(2)
    ev_p(1, 1)
    ev_b2(3)
    toward_step(0)
    ev_m(2, 0)
    ev_m(1, 2)
    ev_b1(3)
    ev_p(3, 0)
    ev_m(2, 3)
    ev_p(2, 0)
    ev_c(2)
    ev_e(1, 2)
    ev_m(1, 1)
    ev_p(1, 2)
    rs_0(0)
    ev_e(1, 1)
    ev_c(1)
    toward_step(1)
    ev_e(1, 0)
    ev_e(1, 3)
    ev_m(2, 1)
    ev_e(2, 1)
    ev_e(2, 2)
    rs_0(1)
    toward_step(2)
    ev_f(1)
    rs_0(2)
    ev_m(3, 0)
    ev_c(3)
    gate_step(1)
    ev_p(2, 2)
    rs_1()
    ev_p(2, 1)
    ev_p(2, 3)
    ev_m(2, 2)
    ev_p(3, 2)
    ev_e(2, 3)
    up_step(1)
    ev_e(3, 0)
    ev_p(3, 1)
    ev_f(2)
    ev_p(3, 3)
    ev_m(3, 2)
    back_step(1)
    gate_step(2)
    rs_2()
    ev_e(3, 1)
    up_step(2)
    ev_m(3, 3)
    ev_m(3, 1)
    ev_e(3, 2)
    ev_e(3, 3)
    back_step(2)
    ev_f(3)
    gate_step(3)
    rs_3()
    up_step(3)
    rs_4()
    back_step(3)
    rs_5()
    rs_6()
    await_shared()
    act_copy(2).wait()
    act_copy(3).wait()
    for s in range(4):
        for a in range(2):
            pltpu.make_async_copy(
                xx.at[a, s, pl.ds(0, 4 * rows), :],
                own_hbm.at[a, :, pl.ds(s * toks, toks)],
                own_sem.at[a, s],
            ).wait()
        sent = 15 if s in (0, 3) else 9
        await_(xx.at[0, s, pl.ds(0, sent * rows), :], send_sem.at[s])
        await_(xx.at[0, s], sib_send_sem.at[s])
    await_(z_sib, misc_send.at[0])
    await_(xx.at[0, 0, pl.ds(0, 3 * rows), :], misc_send.at[1])
    await_(levels.at[pl.ds(0, 3)], misc_send.at[2])
    await_(part_sib, misc_send.at[3])
    await_(line_two, misc_send.at[4])
    await_(line_four, misc_send.at[5])
    await_(block_half, misc_send.at[6])
    await_(block_one, misc_send.at[7])
    await_(fin_sib, misc_send.at[8])
    await_(xx.at[0, 0, pl.ds(0, 12 * rows), :], misc_send.at[9])
    await_(shared(0), misc_send.at[10])
    await_(shared(0), misc_send.at[11])


def layer(tokens, cotangent, prefix, gate_weight, up_weight, down_weight):
    feats, toks = tokens.shape
    width, local = gate_weight.shape
    rows = 2 * feats
    dma = pltpu.SemaphoreType.DMA
    any_ = pl.BlockSpec(memory_space=pltpu.HBM)
    vmem = pl.BlockSpec(memory_space=pltpu.VMEM)
    return pl.pallas_call(
        layer_kernel,
        out_shape=(
            jax.ShapeDtypeStruct((3, 4 * toks, local), BF),
            jax.ShapeDtypeStruct((2, 4 * rows, 4 * toks), BF),
            jax.ShapeDtypeStruct((feats, toks), BF),
            jax.ShapeDtypeStruct((feats, toks), BF),
        ),
        in_specs=[vmem, vmem, pl.BlockSpec(memory_space=pltpu.SMEM), any_, any_, any_],
        out_specs=(any_, any_, vmem, vmem),
        scratch_shapes=[
            pltpu.VMEM((width, local), BF),
            pltpu.VMEM((width, local), BF),
            pltpu.VMEM((local, width), BF),
            pltpu.VMEM((2, 4, width, toks), BF),
            pltpu.VMEM((2, feats, toks), BF),
            pltpu.VMEM((4, 8, 128), jnp.int32),
            pltpu.VMEM((toks, local), F32),
            pltpu.VMEM((toks, local), F32),
            pltpu.VMEM((2, 3, toks, local), BF),
            pltpu.VMEM((2, width, toks), BF),
            pltpu.VMEM((width, toks), BF),
            pltpu.VMEM((2, 2, rows, toks), BF),
            pltpu.VMEM((2, 4, rows, toks), BF),
            pltpu.VMEM((rows, toks), BF),
            pltpu.VMEM((2, rows, toks), BF),
            pltpu.VMEM((2, feats, toks), F32),
            pltpu.VMEM((feats, toks), F32),
            dma((3,)),
            dma((2,)),
            dma((3,)),
            dma((4,)),
            dma((4, 4)),
            dma((4, 12)),
            dma((4, 4)),
            dma((4,)),
            dma((4,)),
            dma((12,)),
            dma((20,)),
            dma((4,)),
            dma((2, 4)),
            dma((2,)),
        ],
        compiler_params=pltpu.CompilerParams(
            collective_id=0, has_side_effects=True, vmem_limit_bytes=67043328
        ),
        name="layer",
    )(tokens, cotangent, prefix, gate_weight, up_weight, down_weight)


def grads_kernel(
    own_hbm,
    acts_hbm,
    first_hbm,
    second_hbm,
    gate_out,
    up_out,
    down_out,
    first_out,
    second_out,
    own,
    acts,
    done,
    small,
    in_sem,
    out_sem,
    small_sem,
):
    half = own.shape[2] // 2
    halves = (pl.ds(0, half), pl.ds(half, half))

    def own_load(a, j):
        return pltpu.make_async_copy(
            own_hbm.at[a, :, halves[j]], own.at[a, :, halves[j]], in_sem.at[2 * a + j]
        )

    def acts_load(k, j):
        return pltpu.make_async_copy(
            acts_hbm.at[k, halves[j]], acts.at[k, halves[j]], in_sem.at[4 + 2 * k + j]
        )

    for k in range(3):
        for j in range(2):
            if k != 1:
                own_load(k // 2, j).start()
            acts_load(k, j).start()
    brought = [
        pltpu.make_async_copy(src, small.at[j], small_sem.at[j])
        for j, src in enumerate((first_hbm, second_hbm))
    ]
    taken = [
        pltpu.make_async_copy(small.at[j], dst, small_sem.at[j])
        for j, dst in enumerate((first_out, second_out))
    ]
    for copy in brought:
        copy.start()
    outs = (gate_out, up_out, down_out)
    stores = [pltpu.make_async_copy(done.at[k], outs[k], out_sem.at[k]) for k in range(3)]

    @pl.loop(0, 3)
    def _(k):
        a = k // 2
        value = None
        for j in range(2):

            @pl.when(k != 1)
            def _():
                own_load(a, j).wait()

            acts_load(k, j).wait()
            term = jnp.dot(
                own[a, :, halves[j]], acts[k, halves[j], :], preferred_element_type=F32
            )
            value = term if value is None else value + term
        done[k] = value.astype(BF)
        for i in range(3):

            @pl.when(k == i)
            def _():
                stores[i].start()
                if i == 0:
                    for copy in brought:
                        copy.wait()
                    for copy in taken:
                        copy.start()

    for copy in stores + taken:
        copy.wait()


def weight_grads(acts, own, first, second):
    kinds, toks, local = acts.shape
    feats = own.shape[1]
    grad = jax.ShapeDtypeStruct((feats, local), BF)
    like = jax.ShapeDtypeStruct(first.shape, BF)
    hbm = pl.BlockSpec(memory_space=pltpu.HBM)
    return pl.pallas_call(
        grads_kernel,
        out_shape=(grad, grad, grad, like, like),
        in_specs=[hbm] * 4,
        out_specs=(hbm,) * 5,
        scratch_shapes=[
            pltpu.VMEM((2, feats, toks), BF),
            pltpu.VMEM((kinds, toks, local), BF),
            pltpu.VMEM((kinds, feats, local), BF),
            pltpu.VMEM((2, *first.shape), BF),
            pltpu.SemaphoreType.DMA((10,)),
            pltpu.SemaphoreType.DMA((3,)),
            pltpu.SemaphoreType.DMA((2,)),
        ],
        compiler_params=pltpu.CompilerParams(vmem_limit_bytes=67043328),
        name="weight_grads",
    )(own, acts, first, second)


def body(tokens, cotangent, prefix, gate_weight, up_weight, down_weight):
    acts, own, output, input_grad = layer(
        tokens.T, cotangent.T, prefix, gate_weight, up_weight, down_weight
    )
    grad_gate, grad_up, grad_down, output, input_grad = weight_grads(
        acts, own, output, input_grad
    )
    return output.T, input_grad.T, grad_gate, grad_up, grad_down.T


def solution(mesh):
    return jax.shard_map(
        body,
        mesh=mesh,
        in_specs=(
            P("dp", "col"),
            P("dp", "col"),
            P("dp"),
            P(None, "col"),
            P(None, "col"),
            P("col", None),
        ),
        out_specs=(P("dp", "col"), P("dp", "col"), P("dp", "col"), P("dp", "col"), P("col", "dp")),
        check_vma=False,
    )
```
